256 devices in a mesh: req: 32 (over x, z), mdl: 8 (over y, core).
Axes of the slice: x: 4, y: 4, z: 8, core: 2. Of those that a mesh axis runs over, the one named last changes fastest.
Arguments:
- hidden_state: bfloat16 [1024, 2880], P('req'), may hold values from -6 to 6
- cached_length_list: int32 [1024], P('req'), may hold values from 1 to 2047, as said below
- page_table: int32 [1024, 16], P('req'), may hold values from 0 to 5631, as said below
- paged_cache_store: bfloat16 [5632, 128, 1024], P('req', None, 'mdl'), may hold values from -68 to 68, as said below
- attention_gain: float32 [2880], replicated, may hold values from 0.5 to 1.5
- qkv_weight: bfloat16 [2880, 5120], P('req', 'mdl'), may hold values from -0.109375 to 0.109375
- qkv_bias: float32 [5120], P('mdl'), may hold values from -3 to 3
- sink_logit_values: float32 [64], P('mdl'), may hold values from -1 to 4
- output_weight: bfloat16 [4096, 2880], P('mdl', 'req'), may hold values from -0.25 to 0.25
- output_bias: float32 [2880], replicated, may hold values from -3 to 3
- expert_gain: float32 [2880], replicated, may hold values from 0.5 to 1.5
- router_weight: bfloat16 [2880, 32], replicated, may hold values from -0.109375 to 0.109375
- router_bias: float32 [32], replicated, may hold values from -4 to 4
- expert_routes: int32 [1024, 4], P('req'), may hold values from 0 to 31, all different within a row; in each aligned block of 32 rows (0 to 31, 32 to 63, ...) at most 8 rows name the same one
- expand_weight: bfloat16 [32, 2880, 5760], P('req', None, 'mdl'), may hold values from -0.109375 to 0.109375
- expand_bias: float32 [32, 5760], P('req', 'mdl'), may hold values from -10 to 10
- reduce_weight: bfloat16 [32, 2880, 2880], P('req', 'mdl'), may hold values from -0.109375 to 0.109375
- reduce_bias: float32 [32, 2880], replicated, may hold values from -3 to 3
Outputs:
- layer_output: bfloat16 [1024, 2880], P('req', 'mdl')
The draws below stay inside these ranges and needn't reach their ends.
Inputs may be any that keep to these rules, and one draw needn't show every extreme that they name: `cached_length_list`: requests r and r + 1 within a block of 32 requests share an owner; about one request in eight holds between 1536 and 2047 cached positions, at most 8 of each owner's 32, and the others at most 256; some owner, and the last owner, hold exactly 8 long ones. `page_table`: the entries of request r name pages of its owner's block, pages r // 32 * 176 to that plus 176 - 1; the pages that hold cached positions differ between requests; entries past a request's last used page are to be ignored. `paged_cache_store`: keys are stored rotated at their own positions. `expert_routes`: each token names 4 different experts; of the rows of one index of req no expert is named by more than 8.
All inputs are finite; a program needn't handle non-finite values.
Results may differ from the reference program's by a relative error of at most 0.024.
Values may be sent and summed in bfloat16 or wider, within the bound.
A program may use at most 192 MiB of HBM per device.

```python
import math
import jax
import jax.numpy as jnp
import numpy as np
from jax import lax

D = 2880
QUERY_HEADS = 64
KEY_VALUE_HEADS = 8
HEAD_SIZE = 64
FF = 2880
TOPK = 4
REQ_DEV = 32
MAX_LEN = 2048
PAGE_POSITIONS = 128
SHORT_MAX = 256
QUERY_PER_KEY = 8
PAGES_PER_REQ = 16
SHORT_PAGES = 2
LONG_MOST = 8
POOL_DEV = 176
TOTAL_PAGES = 5632
REQUEST_COUNT = 1024
EXPERTS = 32
CAP = 8
QKV_COLS = 5120
N_REQ = 32


def request_layout(key):
    base_key = jax.random.fold_in(key, 7)
    key_list = jax.random.split(base_key, 6)
    long_counts = jax.random.randint(key_list[0], (N_REQ,), 0, LONG_MOST + 1)
    busiest = jax.random.randint(key_list[1], (), 0, N_REQ)
    owners = jnp.arange(N_REQ)
    long_counts = jnp.where((owners == busiest) | (owners == N_REQ - 1), LONG_MOST, long_counts)
    orders = jax.vmap(lambda sub_key: jax.random.permutation(sub_key, REQ_DEV))(jax.random.split(key_list[2], N_REQ))
    ranks = jnp.argsort(orders, axis=1)
    is_long = ranks < long_counts[:, None]
    short_lengths = jax.random.randint(key_list[3], (N_REQ, REQ_DEV), 1, SHORT_MAX + 1)
    long_lengths = jax.random.randint(key_list[4], (N_REQ, REQ_DEV), MAX_LEN - MAX_LEN // 4, MAX_LEN)
    lengths = jnp.where(is_long, long_lengths, short_lengths)
    on_busiest = (owners == busiest)[:, None]
    lengths = jnp.where(on_busiest & (ranks == 0), MAX_LEN - 1, lengths)
    lengths = jnp.where(on_busiest & (ranks == REQ_DEV - 1), 1, lengths)
    capacity = jnp.where(is_long, PAGES_PER_REQ, SHORT_PAGES)
    offsets = jnp.cumsum(capacity, axis=1) - capacity
    pool_orders = jax.vmap(lambda sub_key: jax.random.permutation(sub_key, POOL_DEV))(jax.random.split(key_list[5], N_REQ))
    columns = jnp.minimum(jnp.arange(PAGES_PER_REQ)[None, None, :], capacity[:, :, None] - 1) + offsets[:, :, None]
    picked = pool_orders[owners[:, None, None], columns]
    page_numbers = owners[:, None, None] * POOL_DEV + picked
    return (lengths.reshape(REQUEST_COUNT).astype(jnp.int32), page_numbers.reshape(REQUEST_COUNT, PAGES_PER_REQ).astype(jnp.int32))


def draw_cached_length_list(key, part):
    return request_layout(key)[0]


def draw_page_table(key, part):
    return request_layout(key)[1]


def draw_paged_cache_store(key, part):
    value_rows = jnp.clip(jax.random.normal(key, (TOTAL_PAGES, PAGE_POSITIONS, KEY_VALUE_HEADS, 2, HEAD_SIZE), jnp.float32), -6.0, 6.0)
    return value_rows.reshape(TOTAL_PAGES, PAGE_POSITIONS, KEY_VALUE_HEADS * 2 * HEAD_SIZE).astype(jnp.bfloat16)


def block_scale(stream_key, shape, cuts, least, high):
    level = 1.0
    for position, parts in cuts:
        heights = jax.random.uniform(jax.random.fold_in(jax.random.fold_in(stream_key, 6), position), (parts,), jnp.float32, least / len(cuts), high / len(cuts))
        level = level * jnp.repeat(jnp.exp(heights), shape[position] // parts).reshape((-1,) + (1,) * (len(shape) - 1 - position))
    return level


def shared_out(stream_key, own, number, rows, amount, top, most, slope):
    ranking = jax.random.permutation(stream_key, amount)
    heavy_load, usual = portions_of(amount, rows * top, most, slope, True), portions_of(amount, rows * top, most, slope, False)
    places = jnp.arange(amount)

    def named(sizes, offset_by):
        used = int((sizes > 0).sum())
        fixed = max(1, used // 4)
        moved = fixed + (places - fixed + offset_by * (used - fixed)) % max(1, amount - fixed)
        return jnp.zeros((amount,), jnp.int32).at[ranking[jnp.where(places < fixed, places, moved)]].set(jnp.asarray(sizes, jnp.int32))

    sizes = jnp.where(number % 4 == 0, named(heavy_load, number // 4), named(usual, number - number // 4 - 1))
    mixed = jax.random.permutation(jax.random.fold_in(own, 3), amount)
    source_of, taker = mixed[0:amount // 2 * 2:2], mixed[1:amount // 2 * 2:2]
    margin = jnp.minimum(sizes[source_of] - 1, most - sizes[taker]) // 2
    margin = jnp.where((source_of == ranking[0]) | (taker == ranking[0]) | (sizes[taker] == 0), 0, jnp.maximum(margin, 0))
    moved = jax.random.randint(jax.random.fold_in(own, 4), (amount // 2,), 0, 1 << 20) % (margin + 1)
    sizes = sizes.at[source_of].add(-moved).at[taker].add(moved)
    members = jnp.searchsorted(jnp.cumsum(sizes), jnp.arange(rows * top), side="right").astype(jnp.int32)
    listing = members.reshape(top, rows).T
    listing = listing[jax.random.permutation(jax.random.fold_in(own, 1), rows)]
    offset_by = jax.random.randint(jax.random.fold_in(own, 2), (rows, 1), 0, top)
    return jnp.take_along_axis(listing, (jnp.arange(top)[None, :] + offset_by) % top, axis=1)


def portions_of(number_of, total, limit, skew, full):
    loads = [(1 << 20) // math.isqrt(rank ** skew) + 1 for rank in range(1, number_of + 1)]
    largest = limit if full else min(limit, max(-(-total // number_of), total * loads[0] // sum(loads)))
    least = 1 if total - largest >= number_of - 1 else 0
    holding, rest = [largest] + [least] * (number_of - 1), total - largest - least * (number_of - 1)
    while rest > 0:
        candidates = [i for i in range(1, number_of) if holding[i] < largest] or [i for i in range(1, number_of) if holding[i] < limit]
        pool, left = sum([loads[i] for i in candidates]), rest
        for i in candidates:
            extra = min(limit - holding[i], max(1, left * loads[i] // pool), rest)
            holding[i] = holding[i] + extra
            rest = rest - extra
    return np.array(holding)


def normal_values(stream_key, shape, scale, limit, shards=(), held_as=jnp.bfloat16):
    values = scale * jax.random.normal(stream_key, shape, jnp.float32)
    if shards:
        values = values * block_scale(stream_key, shape, shards, -0.22, 0.18)
    return jnp.clip(values, -limit, limit).astype(held_as)


def setup_inputs(seed: int = 0) -> dict:
    keys = jax.random.split(jax.random.key(seed), 19)
    hidden_state = normal_values(keys[0], (REQUEST_COUNT, D), 1.0, 6.0, ((0, 32),))
    cached_length_list = draw_cached_length_list(jax.random.fold_in(keys[18], 71), 0)
    page_table = draw_page_table(jax.random.fold_in(keys[18], 71), 0)
    paged_cache_store = draw_paged_cache_store(jax.random.fold_in(keys[18], 71), 0)
    attention_gain = jnp.clip(1.0 + 0.1 * jax.random.normal(keys[4], (D,), jnp.float32), 0.5, 1.5)
    qkv_weight = normal_values(keys[5], (D, QKV_COLS), D ** -0.5, 0.109375, ((0, 32), (1, 8)))
    qkv_bias = normal_values(keys[6], (QKV_COLS,), 0.5, 3.0, ((0, 8),), jnp.float32)
    sink_logit_values = jnp.clip(-1.0 + 5.0 * jax.random.uniform(keys[7], (QUERY_HEADS,), jnp.float32) ** block_scale(keys[7], (QUERY_HEADS,), ((0, 8),), -0.2, 0.2), -1.0, 4.0)
    output_weight = normal_values(keys[8], (QUERY_HEADS * HEAD_SIZE, D), (QUERY_HEADS * HEAD_SIZE // 8) ** -0.5, 0.25, ((0, 8), (1, 32)))
    output_bias = normal_values(keys[9], (D,), 0.5, 3.0, (), jnp.float32)
    expert_gain = jnp.clip(1.0 + 0.1 * jax.random.normal(keys[10], (D,), jnp.float32), 0.5, 1.5)
    router_weight = normal_values(keys[11], (D, EXPERTS), D ** -0.5, 0.109375)
    router_bias = normal_values(keys[12], (EXPERTS,), 1.0, 4.0, (), jnp.float32)
    expert_routes_keys = jax.random.split(jax.random.fold_in(keys[13], 1), REQUEST_COUNT // REQ_DEV)
    expert_routes_turns = jax.random.permutation(jax.random.fold_in(keys[13], 3), REQUEST_COUNT // REQ_DEV)
    expert_routes = jax.vmap(lambda own, number: shared_out(jax.random.fold_in(keys[13], 2), own, number, REQ_DEV, EXPERTS, TOPK, CAP, 2))(expert_routes_keys, expert_routes_turns).reshape((REQUEST_COUNT, TOPK))
    expand_weight = normal_values(keys[14], (EXPERTS, D, 2 * FF), D ** -0.5, 0.109375, ((0, 32), (2, 8)))
    expand_bias = normal_values(keys[15], (EXPERTS, 2 * FF), 2.5, 10.0, ((0, 32), (1, 8)), jnp.float32)
    reduce_weight = normal_values(keys[16], (EXPERTS, FF, D), FF ** -0.5, 0.109375, ((0, 32), (1, 8)))
    reduce_bias = normal_values(keys[17], (EXPERTS, D), 0.5, 3.0, (), jnp.float32)
    return {"hidden_state": hidden_state, "cached_length_list": cached_length_list, "page_table": page_table, "paged_cache_store": paged_cache_store, "attention_gain": attention_gain, "qkv_weight": qkv_weight, "qkv_bias": qkv_bias, "sink_logit_values": sink_logit_values, "output_weight": output_weight, "output_bias": output_bias, "expert_gain": expert_gain, "router_weight": router_weight, "router_bias": router_bias, "expert_routes": expert_routes, "expand_weight": expand_weight, "expand_bias": expand_bias, "reduce_weight": reduce_weight, "reduce_bias": reduce_bias}


norm_epsilon = 1e-05
rope_theta = 150000.0
swiglu_limit = 7.0
swiglu_alpha = 1.702

def normalize(row_values, gain):
    value_rows = row_values.astype(jnp.float32)
    mean_square = lax.optimization_barrier(jnp.mean(value_rows * value_rows, axis=-1, keepdims=True))
    return value_rows * lax.rsqrt(mean_square + norm_epsilon) * gain

def apply_rotation(value_rows, positions):
    half_width = value_rows.shape[-1] // 2
    exponent = jnp.arange(half_width, dtype=jnp.float32) * (2.0 / value_rows.shape[-1])
    frequency = jnp.power(rope_theta, -exponent)
    angles = positions.astype(jnp.float32)[:, None] * frequency[None, :]
    cosine = jnp.cos(angles)[:, None, :]
    sine_part = jnp.sin(angles)[:, None, :]
    first_half = value_rows[..., :half_width]
    second_half = value_rows[..., half_width:]
    return jnp.concatenate([first_half * cosine - second_half * sine_part, second_half * cosine + first_half * sine_part], axis=-1)

def expert_rows(inputs, expand_local, expand_local_bias, reduce_local):
    pre_activation = jnp.dot(inputs, expand_local, preferred_element_type=jnp.float32) + expand_local_bias
    gate_part = jnp.minimum(pre_activation[:, 0::2], swiglu_limit)
    up_part = jnp.clip(pre_activation[:, 1::2], -swiglu_limit, swiglu_limit)
    activation = (gate_part * jax.nn.sigmoid(swiglu_alpha * gate_part) * (up_part + 1.0)).astype(jnp.bfloat16)
    return jnp.dot(activation, reduce_local, preferred_element_type=jnp.float32)

def reference(hidden_state, cached_length_list, page_table, paged_cache_store, attention_gain, qkv_weight, qkv_bias, sink_logit_values, output_weight, output_bias, expert_gain, router_weight, router_bias, expert_routes, expand_weight, expand_bias, reduce_weight, reduce_bias):
    normed = normalize(hidden_state, attention_gain).astype(jnp.bfloat16)
    projected_rows = jnp.dot(normed, qkv_weight, preferred_element_type=jnp.float32) + qkv_bias
    projected_rows = projected_rows.reshape(REQUEST_COUNT, KEY_VALUE_HEADS, QUERY_PER_KEY + 2, HEAD_SIZE)
    query_rows = apply_rotation(projected_rows[:, :, :QUERY_PER_KEY].reshape(REQUEST_COUNT, QUERY_HEADS, HEAD_SIZE), cached_length_list).astype(jnp.bfloat16).reshape(REQUEST_COUNT, KEY_VALUE_HEADS, QUERY_PER_KEY, HEAD_SIZE)
    new_keys = apply_rotation(projected_rows[:, :, QUERY_PER_KEY], cached_length_list).astype(jnp.bfloat16)
    new_values = projected_rows[:, :, QUERY_PER_KEY + 1].astype(jnp.bfloat16)
    cache_page_store = paged_cache_store.reshape(TOTAL_PAGES, PAGE_POSITIONS, KEY_VALUE_HEADS, 2, HEAD_SIZE)
    sink_logit_table = sink_logit_values.reshape(KEY_VALUE_HEADS, QUERY_PER_KEY)
    score_scale = 1.0 / math.sqrt(HEAD_SIZE)

    def attend_one(request):
        query_row, key_row, value_row, length, page_numbers = request
        cached_entries = cache_page_store[page_numbers].reshape(PAGES_PER_REQ * PAGE_POSITIONS, KEY_VALUE_HEADS, 2, HEAD_SIZE).astype(jnp.float32)
        query_wide = query_row.astype(jnp.float32)
        scores = jnp.einsum('hgd,lhd->hgl', query_wide, cached_entries[:, :, 0]) * score_scale
        own_score = jnp.einsum('hgd,hd->hg', query_wide, key_row.astype(jnp.float32)) * score_scale
        is_live = jnp.arange(PAGES_PER_REQ * PAGE_POSITIONS) < length
        scores = jnp.where(is_live[None, None, :], scores, -jnp.inf)
        largest = jnp.maximum(jnp.maximum(lax.optimization_barrier(jnp.max(scores, axis=-1)), own_score), sink_logit_table)
        cached_weight = jnp.exp(scores - largest[..., None])
        own_weight = jnp.exp(own_score - largest)
        denominator = lax.optimization_barrier(jnp.sum(cached_weight, axis=-1)) + own_weight + jnp.exp(sink_logit_table - largest)
        cached_share = (cached_weight / denominator[..., None]).astype(jnp.bfloat16)
        own_share = (own_weight / denominator).astype(jnp.bfloat16)
        mixture = jnp.einsum('hgl,lhd->hgd', cached_share.astype(jnp.float32), cached_entries[:, :, 1])
        mixture = mixture + own_share.astype(jnp.float32)[..., None] * value_row.astype(jnp.float32)[:, None, :]
        return mixture.astype(jnp.bfloat16).reshape(QUERY_HEADS * HEAD_SIZE)
    attended = lax.map(attend_one, (query_rows, new_keys, new_values, cached_length_list, page_table))
    residual = (hidden_state.astype(jnp.float32) + jnp.dot(attended, output_weight, preferred_element_type=jnp.float32) + output_bias).astype(jnp.bfloat16)
    expert_input = normalize(residual, expert_gain).astype(jnp.bfloat16)
    logits = jnp.dot(expert_input, router_weight, preferred_element_type=jnp.float32) + router_bias
    chosen = jnp.take_along_axis(logits, expert_routes, axis=1)
    gate_weights = jax.nn.softmax(chosen, axis=-1)
    pair_expert = expert_routes.reshape(-1)
    row_bound = N_REQ * CAP

    def expert_step(totals, expert):
        matches = pair_expert == expert
        row_ids = jnp.nonzero(matches, size=row_bound, fill_value=0)[0]
        is_valid = jnp.arange(row_bound) < jnp.sum(matches.astype(jnp.int32))
        inputs = expert_input[row_ids // TOPK]
        outputs = expert_rows(inputs, expand_weight[expert], expand_bias[expert], reduce_weight[expert])
        outputs = jnp.where(is_valid[:, None], outputs, 0.0)
        return (totals.at[row_ids].add(outputs), None)
    totals, unused = lax.scan(expert_step, jnp.zeros((REQUEST_COUNT * TOPK, D), jnp.float32), jnp.arange(EXPERTS))
    routed = totals.reshape(REQUEST_COUNT, TOPK, D) + reduce_bias[expert_routes]
    blended = lax.optimization_barrier(jnp.sum(gate_weights[:, :, None] * routed, axis=1))
    return (residual.astype(jnp.float32) + blended).astype(jnp.bfloat16)
```

```python
import functools
import math

import jax
import jax.numpy as jnp
from jax import lax
from jax.experimental import pallas as pl
from jax.experimental.pallas import tpu as pltpu
from jax.sharding import PartitionSpec as P

HEAD_SIZE = 64
PAGE_POSITIONS = 128
SHORT_MAX = 256
QUERY_PER_KEY = 8
SHORT_PAGES = 2
SLOTS = 8

NX, NZ, NY, NC = 4, 8, 4, 2

norm_epsilon = 1e-05
rope_theta = 150000.0
swiglu_limit = 7.0
swiglu_alpha = 1.702

BF = jnp.bfloat16
F32 = jnp.float32
VMEM_LIMIT = 58 * 2**20
MESH = pl.DeviceIdType.MESH


def place():
    r = lax.axis_index("req")
    m = lax.axis_index("mdl")
    return r, m, r // NZ, r % NZ, m // NC, m % NC


def device(r, m):
    return {"req": r, "mdl": m}


def dot(a, b):
    return jnp.dot(a, b, preferred_element_type=F32)


def dot_nt(a, b):
    return lax.dot_general(a, b, (((1,), (1,)), ((), ())), preferred_element_type=F32)


def split3(value):
    high = value.astype(BF)
    rest = value - high.astype(F32)
    middle = rest.astype(BF)
    low = (rest - middle.astype(F32)).astype(BF)
    return high, middle, low


class Ring:
    def __init__(self, size, me, ref_of, send, recv, target):
        self.size, self.me, self.ref_of = size, me, ref_of
        self.send, self.recv, self.target = send, recv, target
        self.half = size // 2
        self.plan = [
            (way, dist, part)
            for dist in range(1, self.half + 1)
            for part in range(2)
            for way in range(2)
            if self.exists(way, dist, part)
        ]

    def exists(self, way, dist, part):
        return dist < self.half or (dist == self.half and part == way)

    def index(self, way, dist, part):
        return (way * self.half + dist - 1) * 2 + part

    def origin(self, way, dist):
        return (self.me + (dist if way else self.size - dist)) % self.size

    def copy(self, way, dist, part):
        ref = self.ref_of(self.origin(way, dist - 1), part)
        i = self.index(way, dist, part)
        to = (self.me + (self.size - 1 if way else 1)) % self.size
        return pltpu.make_async_remote_copy(
            src_ref=ref,
            dst_ref=ref,
            send_sem=self.send.at[i],
            recv_sem=self.recv.at[i],
            device_id=self.target(to),
            device_id_type=MESH,
        )

    def arrive(self, way, dist, part):
        ref = self.ref_of(self.origin(way, dist), part)
        i = self.index(way, dist, part)
        pltpu.make_async_remote_copy(
            src_ref=ref,
            dst_ref=ref,
            send_sem=self.send.at[i],
            recv_sem=self.recv.at[i],
            device_id=self.target(self.me),
            device_id_type=MESH,
        ).wait_recv()

    def begin(self, part):
        for way in range(2):
            if self.exists(way, 1, part):
                self.copy(way, 1, part).start()

    def step(self, way, dist, part):
        self.arrive(way, dist, part)
        if self.exists(way, dist + 1, part):
            self.copy(way, dist + 1, part).start()

    def finish(self):
        for way, dist, part in self.plan:
            self.copy(way, dist, part).wait_send()


def remote(src, dst, send, recv, r, m):
    return pltpu.make_async_remote_copy(
        src_ref=src,
        dst_ref=dst,
        send_sem=send,
        recv_sem=recv,
        device_id=device(r, m),
        device_id_type=MESH,
    )


def ring_sems(size):
    return [pltpu.SemaphoreType.DMA((2 * size,)), pltpu.SemaphoreType.DMA((2 * size,))]


def lane_cut(width):
    tiles = width // 128
    return 128 * ((tiles + 1) // 2) if tiles > 1 else 0


def project_kernel(
    hidden, gain, wqkv, wo, bias,
    proj, wo_out,
    gathered, wo_all, parcels, rows, blocks, total, sums, sums_in,
    ring_send, ring_recv, wo_send, wo_recv, x_send, x_recv, s_send, s_recv, local,
):
    r, m, x, z, y, c = place()
    tokens, width = hidden.shape
    group = width // NX
    block = group // NZ

    load_q = pltpu.make_async_copy(wqkv, gathered.at[z], local.at[0])
    load_o = pltpu.make_async_copy(wo, wo_all.at[z], local.at[1])
    load_q.start()
    load_o.start()

    barrier = pltpu.get_barrier_semaphore()
    for step in (1, NZ - 1):
        pl.semaphore_signal(barrier, inc=1, device_id=device(x * NZ + (z + step) % NZ, m), device_id_type=MESH)
    for step in range(1, NX):
        pl.semaphore_signal(barrier, inc=1, device_id=device((x + step) % NX * NZ + z, m), device_id_type=MESH)
    load_q.wait()
    pl.semaphore_wait(barrier, NX + 1)

    cut_q, cut_o = lane_cut(wqkv.shape[1]), lane_cut(wo.shape[1])

    def part_of(buffer, cut):
        full = buffer.shape[-1]

        def ref_of(origin, part):
            return buffer.at[origin, :, pl.ds(0, cut) if part == 0 else pl.ds(cut, full - cut)]

        return ref_of

    def at_z(to):
        return device(x * NZ + to, m)

    ring = Ring(NZ, z, part_of(gathered, cut_q), ring_send, ring_recv, at_z)
    ring_o = Ring(NZ, z, part_of(wo_all, cut_o), wo_send, wo_recv, at_z)
    for part in range(2):
        ring.begin(part)

    value = hidden[...].astype(F32)
    scale = lax.rsqrt(jnp.mean(value * value, axis=-1, keepdims=True) + norm_epsilon)
    normed = (value * scale * gain[...]).astype(BF)
    for k in range(NX):
        parcels[k] = normed[:, group * k : group * k + group]

    def x_copy(src, dst, send, recv, step):
        to = (x + step) % NX
        return remote(src.at[to], dst.at[x], send.at[step], recv.at[step], to * NZ + z, m)

    def x_arrive(dst, send, recv, step):
        origin = (x + NX - step) % NX
        remote(dst.at[origin], dst.at[origin], send.at[step], recv.at[step], r, m).wait_recv()

    for step in range(1, NX):
        x_copy(parcels, rows, x_send, x_recv, step).start()
    rows[x] = parcels[x]

    for step in range(1, NX):
        x_arrive(rows, x_send, x_recv, step)
    for k in range(NZ):
        for j in range(NX):
            blocks[k, j * tokens : (j + 1) * tokens] = rows[j, :, block * k : block * k + block]

    def add(origin, first):
        product = dot(blocks[origin], gathered[origin])
        for j in range(NX):
            piece = product[j * tokens : (j + 1) * tokens]
            total[j] = piece if first else total[j] + piece

    add(z, True)
    for dist in range(1, ring.half + 1):
        for way, d, part in ring.plan:
            if d == dist:
                ring.step(way, d, part)
        if dist == ring.half - 1 or ring.half == 1:
            load_o.wait()
            for part in range(2):
                ring_o.begin(part)
        add(ring.origin(0, dist), False)
        if dist < ring.half:
            add(ring.origin(1, dist), False)

    for j in range(NX):
        sums[j] = total[j].astype(BF)
    for step in range(1, NX):
        x_copy(sums, sums_in, s_send, s_recv, step).start()
    for way, dist, part in ring_o.plan:
        ring_o.step(way, dist, part)
    result = total[x] + bias[...]
    for step in range(1, NX):
        x_arrive(sums_in, s_send, s_recv, step)
        result = result + sums_in[(x + NX - step) % NX].astype(F32)
    proj[...] = result
    for k in range(NZ):
        wo_out[k] = wo_all[k]

    ring.finish()
    ring_o.finish()
    for step in range(1, NX):
        x_copy(parcels, rows, x_send, x_recv, step).wait_send()
        x_copy(sums, sums_in, s_send, s_recv, step).wait_send()


def project(hidden, gain, wqkv, wo, bias):
    tokens, width = hidden.shape
    group = width // NX
    block, cols = wqkv.shape
    out_rows = wo.shape[1]
    vmem = pl.BlockSpec(memory_space=pltpu.VMEM)
    hbm = pl.BlockSpec(memory_space=pl.ANY)
    return pl.pallas_call(
        project_kernel,
        name="project",
        out_shape=(
            jax.ShapeDtypeStruct((tokens, cols), F32),
            jax.ShapeDtypeStruct((NZ, block, out_rows), BF),
        ),
        in_specs=[vmem, vmem, hbm, hbm, vmem],
        out_specs=(vmem, vmem),
        scratch_shapes=[
            pltpu.VMEM((NZ, block, cols), BF),
            pltpu.VMEM((NZ, block, out_rows), BF),
            pltpu.VMEM((NX, tokens, group), BF),
            pltpu.VMEM((NX, tokens, group), BF),
            pltpu.VMEM((NZ, NX * tokens, block), BF),
            pltpu.VMEM((NX, tokens, cols), F32),
            pltpu.VMEM((NX, tokens, cols), BF),
            pltpu.VMEM((NX, tokens, cols), BF),
            *ring_sems(NZ),
            *ring_sems(NZ),
            *[pltpu.SemaphoreType.DMA((NX,))] * 4,
            pltpu.SemaphoreType.DMA((2,)),
        ],
        compiler_params=pltpu.CompilerParams(
            collective_id=1, has_side_effects=True, vmem_limit_bytes=VMEM_LIMIT
        ),
    )(hidden, gain, wqkv, wo, bias)


def attend_kernel(
    lengths, table, proj, cosines, sines, sinks, cache,
    out,
    short, long, queries, mixed, owns, short_sem, long_sem,
):
    count = proj.shape[0]
    heads = QUERY_PER_KEY
    pages = table.shape[1]
    score_scale = 1.0 / math.sqrt(HEAD_SIZE)

    def fetch(i, used):
        for p in range(SHORT_PAGES):
            pltpu.make_async_copy(
                cache.at[table[i, p]], short.at[i, pl.ds(p * PAGE_POSITIONS, PAGE_POSITIONS)], short_sem.at[i]
            ).start()
        is_long = lengths[i] > SHORT_MAX

        @pl.when(is_long)
        def _():
            for p in range(SHORT_PAGES, pages):
                pltpu.make_async_copy(
                    cache.at[table[i, p]],
                    long.at[used, pl.ds((p - SHORT_PAGES) * PAGE_POSITIONS, PAGE_POSITIONS)],
                    long_sem.at[used],
                ).start()

        return used + is_long.astype(jnp.int32)

    lax.fori_loop(0, count, fetch, jnp.int32(0))

    value = proj[...]
    lanes = lax.broadcasted_iota(jnp.int32, value.shape, 1)
    width = value.shape[1]
    first = (lanes % HEAD_SIZE) < HEAD_SIZE // 2
    partner = jnp.where(
        first,
        pltpu.roll(value, width - HEAD_SIZE // 2, axis=1),
        pltpu.roll(value, HEAD_SIZE // 2, axis=1),
    )
    repeat = width // cosines.shape[1]
    turned = value * jnp.concatenate([cosines[...]] * repeat, axis=1) + partner * jnp.concatenate(
        [sines[...]] * repeat, axis=1
    )
    key_at = heads * HEAD_SIZE
    rounded = jnp.where(lanes < key_at + HEAD_SIZE, turned, value).astype(BF).astype(F32)
    new_key = rounded[:, key_at : key_at + HEAD_SIZE]
    new_value = rounded[:, key_at + HEAD_SIZE :]
    queries[...] = jnp.zeros_like(queries)
    for h in range(heads):
        head = rounded[:, h * HEAD_SIZE : (h + 1) * HEAD_SIZE]
        queries[:, h, 0:HEAD_SIZE] = head
        own = jnp.sum(head * new_key, axis=1, keepdims=True) * score_scale
        owns[:, h, :] = jnp.broadcast_to(own, (count, owns.shape[2]))
    sink = sinks[...]

    def one(i, used):
        length = lengths[i]
        query = queries[i].astype(BF)
        own = owns[i][:, 0:1]
        pltpu.make_async_copy(short.at[i], short.at[i], short_sem.at[i]).wait()
        entries = short[i]
        scores = dot_nt(query, entries) * score_scale
        positions = lax.broadcasted_iota(jnp.int32, scores.shape, 1)
        scores = jnp.where(positions < length, scores, -jnp.inf)
        largest = jnp.maximum(jnp.maximum(jnp.max(scores, axis=1, keepdims=True), own), sink)
        is_long = length > SHORT_MAX

        @pl.when(jnp.logical_not(is_long))
        def _():
            weight = jnp.exp(scores - largest)
            own_weight = jnp.exp(own - largest)
            bottom = jnp.sum(weight, axis=1, keepdims=True) + own_weight + jnp.exp(sink - largest)
            mixed[i] = dot((weight / bottom).astype(BF), entries)
            owns[i] = jnp.broadcast_to((own_weight / bottom).astype(BF).astype(F32), owns.shape[1:])

        @pl.when(is_long)
        def _():
            pltpu.make_async_copy(long.at[used], long.at[used], long_sem.at[used]).wait()
            far = long[used]
            more = dot_nt(query, far) * score_scale
            at = lax.broadcasted_iota(jnp.int32, more.shape, 1) + SHORT_MAX
            more = jnp.where(at < length, more, -jnp.inf)
            top = jnp.maximum(largest, jnp.max(more, axis=1, keepdims=True))
            weight = jnp.exp(scores - top)
            far_weight = jnp.exp(more - top)
            own_weight = jnp.exp(own - top)
            bottom = (
                jnp.sum(weight, axis=1, keepdims=True)
                + jnp.sum(far_weight, axis=1, keepdims=True)
                + own_weight
                + jnp.exp(sink - top)
            )
            mixed[i] = dot((weight / bottom).astype(BF), entries) + dot((far_weight / bottom).astype(BF), far)
            owns[i] = jnp.broadcast_to((own_weight / bottom).astype(BF).astype(F32), owns.shape[1:])

        return used + is_long.astype(jnp.int32)

    lax.fori_loop(0, count, one, jnp.int32(0))
    for h in range(heads):
        head = mixed[:, h, HEAD_SIZE:] + owns[:, h, 0:1] * new_value
        out[:, h * HEAD_SIZE : (h + 1) * HEAD_SIZE] = head.astype(BF)


def attend(lengths, table, proj, cosines, sines, sinks, cache):
    count = proj.shape[0]
    channels = cache.shape[2]
    pages = table.shape[1]
    vmem = pl.BlockSpec(memory_space=pltpu.VMEM)
    smem = pl.BlockSpec(memory_space=pltpu.SMEM)
    most_long = count // 4
    return pl.pallas_call(
        attend_kernel,
        name="attend",
        out_shape=jax.ShapeDtypeStruct((count, QUERY_PER_KEY * HEAD_SIZE), BF),
        in_specs=[smem, smem, vmem, vmem, vmem, vmem, pl.BlockSpec(memory_space=pl.ANY)],
        out_specs=vmem,
        scratch_shapes=[
            pltpu.VMEM((count, SHORT_PAGES * PAGE_POSITIONS, channels), BF),
            pltpu.VMEM((most_long, (pages - SHORT_PAGES) * PAGE_POSITIONS, channels), BF),
            pltpu.VMEM((count, QUERY_PER_KEY, channels), F32),
            pltpu.VMEM((count, QUERY_PER_KEY, channels), F32),
            pltpu.VMEM((count, QUERY_PER_KEY, channels), F32),
            pltpu.SemaphoreType.DMA((count,)),
            pltpu.SemaphoreType.DMA((most_long,)),
        ],
        compiler_params=pltpu.CompilerParams(vmem_limit_bytes=VMEM_LIMIT),
    )(lengths, table, proj, cosines, sines, sinks, cache)


def expert_kernel(
    att, wo_all, hidden, obias, egain, router, router_bias, routes, routes_t, w1_hbm, b1, w2_hbm, rbias,
    out,
    w1, w2, heads, halves, summed, mine, outgoing, gathered, full, pre, near_out, near_in, far_out, far_in,
    kept, back_out, back_in, logits_out, logits_in, share_f32, gains,
    x_send, x_recv, s_send, s_recv, d_send, d_recv, ring_send, ring_recv, p_send, p_recv,
    n_send, n_recv, f_send, f_recv, b_send, b_recv, l_send, l_recv, local,
):
    r, m, x, z, y, c = place()
    tokens, width = hidden.shape
    count_req, count_mdl = NX * NZ, NY * NC
    share = width // count_mdl
    block = width // count_req
    padded = outgoing.shape[2]
    rows = count_req * SLOTS
    per_group = NZ * block // share

    load1 = pltpu.make_async_copy(w1_hbm, w1, local.at[0])
    load2 = pltpu.make_async_copy(w2_hbm, w2, local.at[1])
    load1.start()
    load2.start()

    barrier = pltpu.get_barrier_semaphore()

    def greet(to_r, to_m):
        pl.semaphore_signal(barrier, inc=1, device_id=device(to_r, to_m), device_id_type=MESH)

    def greet_req(step, carry):
        greet((r + step) % count_req, m)
        return carry

    lax.fori_loop(1, count_req, greet_req, 0)
    for step in range(1, count_mdl):
        greet(r, (m + step) % count_mdl)
    diagonal = x == y
    for step in range(NX):
        for j in range(per_group):
            not_me = jnp.logical_or(step > 0, per_group * x + j != m)

            @pl.when(not_me)
            def _():
                greet((x + step) % NX * NZ + z, per_group * x + j)

    for j in range(count_mdl):

        @pl.when(jnp.logical_not(jnp.logical_and(diagonal, m == j)))
        def _():
            greet(y * NZ + z, j)

    pl.semaphore_wait(
        barrier,
        (count_req - 1) + (count_mdl - 1) + NX * per_group + count_mdl - 2 * diagonal.astype(jnp.int32),
    )

    for step in range(1, NX):
        to = (x + step) % NX
        remote(att, heads.at[x], x_send.at[step], x_recv.at[step], to * NZ + z, m).start()
    heads[x] = att[...]

    for k in range(count_mdl):

        @pl.when(m == k)
        def _():
            at = slice(share * k, share * k + share)
            share_f32[...] = hidden[:, at].astype(F32) + obias[:, at]
            gains[0:1, :] = egain[:, at]
            gains[8 : 8 + count_req, :] = rbias[:, at]
            gains[8 + count_req : 8 + 2 * count_req, :] = router[:, at].astype(F32)

    names = lax.broadcasted_iota(jnp.int32, (count_req, tokens), 0)
    hot_t = jnp.zeros((count_req, tokens), F32)
    for k in range(routes_t.shape[0]):
        hot_t = hot_t + (routes_t[k : k + 1, :] == names).astype(F32)
    names = lax.broadcasted_iota(jnp.int32, (tokens, count_req), 1)
    hot = jnp.zeros((tokens, count_req), F32)
    for k in range(routes.shape[1]):
        hot = hot + (routes[:, k : k + 1] == names).astype(F32)
    before = lax.broadcasted_iota(jnp.int32, (tokens, tokens), 0) < lax.broadcasted_iota(
        jnp.int32, (tokens, tokens), 1
    )
    rank_t = dot(hot_t.astype(BF), before.astype(BF))
    after = lax.broadcasted_iota(jnp.int32, (tokens, tokens), 0) > lax.broadcasted_iota(
        jnp.int32, (tokens, tokens), 1
    )
    rank = dot(after.astype(BF), hot.astype(BF))
    spread = (
        lax.broadcasted_iota(jnp.int32, (rows, count_req), 0) // SLOTS
        == lax.broadcasted_iota(jnp.int32, (rows, count_req), 1)
    ).astype(BF)
    spread_t = (
        lax.broadcasted_iota(jnp.int32, (count_req, rows), 1) // SLOTS
        == lax.broadcasted_iota(jnp.int32, (count_req, rows), 0)
    ).astype(BF)
    slot = (lax.broadcasted_iota(jnp.int32, (rows, tokens), 0) % SLOTS).astype(F32)
    place_rows = jnp.where(
        jnp.logical_and(dot(spread, hot_t.astype(BF)) > 0.5, dot(spread, rank_t.astype(BF)) == slot), 1.0, 0.0
    ).astype(BF)
    slot_t = (lax.broadcasted_iota(jnp.int32, (tokens, rows), 1) % SLOTS).astype(F32)
    take_rows = jnp.where(
        jnp.logical_and(dot(hot.astype(BF), spread_t) > 0.5, dot(rank.astype(BF), spread_t) == slot_t), 1.0, 0.0
    )

    for step in range(1, NX):
        origin = (x + NX - step) % NX
        remote(heads.at[origin], heads.at[origin], x_send.at[step], x_recv.at[step], r, m).wait_recv()

    stacked = jnp.concatenate([heads[j] for j in range(NX)], axis=0)
    per_share = share // block
    for k in range(NZ):
        product = dot_nt(stacked, wo_all[k]).astype(BF)
        for j in range(NX):
            halves[k // per_share, j, :, block * (k % per_share) : block * (k % per_share) + block] = product[
                j * tokens : (j + 1) * tokens
            ]

    def sum_copy(step, j):
        to = (x + step) % NX
        i = step * per_group + j
        return remote(
            halves.at[j, to], summed.at[m], s_send.at[i], s_recv.at[m], to * NZ + z, per_group * x + j
        )

    for step in range(NX):
        for j in range(per_group):

            @pl.when(jnp.logical_or(step > 0, per_group * x + j != m))
            def _():
                sum_copy(step, j).start()

    @pl.when(diagonal)
    def _():
        summed[m] = halves[m % per_group, x]

    residual = share_f32[...]
    for j in range(count_mdl):

        @pl.when(jnp.logical_not(jnp.logical_and(diagonal, m == j)))
        def _():
            remote(summed.at[j], summed.at[j], s_send.at[0], s_recv.at[j], r, m).wait_recv()

    total = summed[0].astype(F32)
    for j in range(1, count_mdl):
        total = total + summed[j].astype(F32)
    residual = (residual + total).astype(BF).astype(F32)
    share_f32[...] = residual
    squares = jnp.sum(residual * residual, axis=1, keepdims=True)
    scaled = (residual * gains[0:1, :]).astype(BF)
    mine[...] = jnp.zeros_like(mine)
    mine[:, 0:share] = scaled
    for k, piece in enumerate(split3(squares)):
        mine[:, share + k : share + k + 1] = piece

    outgoing[...] = dot(place_rows, mine[...]).astype(BF).reshape(outgoing.shape)

    def send_row(step, carry):
        to = (r + step) % count_req
        remote(outgoing.at[to], gathered.at[m, r], d_send.at[step], d_recv.at[r], to, m).start()
        return carry

    lax.fori_loop(1, count_req, send_row, 0)
    gathered[m, r] = outgoing[r]

    routing = gains[8 + count_req : 8 + 2 * count_req, :].astype(BF)
    logits_out[...] = jnp.zeros_like(logits_out)
    logits_out[:, 0:count_req] = dot_nt(scaled, routing)
    logits_out[:, count_req : count_req + 1] = squares
    for step in range(1, count_mdl):
        to = (m + step) % count_mdl
        remote(logits_out, logits_in.at[m], l_send.at[step], l_recv.at[step], r, to).start()
    logits_in[m] = logits_out[...]

    part_rows = count_req // 2

    def part_ref(origin, part):
        return gathered.at[origin * NC + c, pl.ds(part * part_rows, part_rows)]

    def at_y(to):
        return device(r, to * NC + c)

    ring = Ring(NY, y, part_ref, ring_send, ring_recv, at_y)

    def pair_index(way, dist):
        return way * ring.half + dist

    def pair_copy(way, dist, part):
        origin = ring.origin(way, dist)
        ref = part_ref(origin, part)
        i = pair_index(way, dist) * 2 + part
        return remote(ref, ref, p_send.at[i], p_recv.at[i], r, y * NC + 1 - c)

    def pair_arrive(way, dist, part):
        ref = gathered.at[ring.origin(way, dist) * NC + 1 - c, pl.ds(part * part_rows, part_rows)]
        i = pair_index(way, dist) * 2 + part
        remote(ref, ref, p_send.at[i], p_recv.at[i], r, m).wait_recv()

    for part in range(2):

        def take(origin, carry):
            @pl.when(origin != r)
            def _():
                remote(gathered.at[m, origin], gathered.at[m, origin], d_send.at[0], d_recv.at[origin], r, m).wait_recv()

            return carry

        lax.fori_loop(part * part_rows, (part + 1) * part_rows, take, 0)
        ring.begin(part)
        pair_copy(0, 0, part).start()

    for way, dist, part in ring.plan:
        ring.step(way, dist, part)
        pair_copy(way, dist, part).start()
    pair_plan = [(0, 0, 0), (0, 0, 1)] + ring.plan
    for way, dist, part in pair_plan:
        pair_arrive(way, dist, part)

    load1.wait()
    load2.wait()
    square_sum = jnp.zeros((rows, 1), F32)
    for k in range(count_mdl):
        piece = gathered[k].reshape(rows, padded)
        full[:, share * k : share * k + share] = piece[:, 0:share]
        for j in range(3):
            square_sum = square_sum + piece[:, share + j : share + j + 1].astype(F32)
    root = lax.rsqrt(square_sum * (1.0 / width) + norm_epsilon)
    columns = w1.shape[0]
    pre[...] = jnp.zeros_like(pre)
    pre[:, 0:columns] = dot_nt(full[...], w1[...]) * root + b1[...]
    raw = pre[...]
    up = jnp.clip(pltpu.roll(raw, raw.shape[1] - 1, axis=1), -swiglu_limit, swiglu_limit)
    gate = jnp.minimum(raw, swiglu_limit)
    act = (gate * jax.nn.sigmoid(swiglu_alpha * gate) * (up + 1.0)).astype(BF)
    hidden_units = columns // 2
    pick = (
        lax.broadcasted_iota(jnp.int32, (raw.shape[1], hidden_units), 0)
        == 2 * lax.broadcasted_iota(jnp.int32, (raw.shape[1], hidden_units), 1)
    ).astype(BF)
    act = dot(act, pick).astype(BF)

    def produce(k):
        return dot(act, w2[:, share * k : share * k + share])

    def near_copy(k):
        return remote(near_out.at[k], near_in.at[k], n_send.at[k], n_recv.at[k], r, y * NC + 1 - c)

    for core in range(NC):

        @pl.when(c == core)
        def _():
            for k in range(NY):
                near_out[k] = produce(k * NC + 1 - core).astype(BF)
                near_copy(k).start()
            for k in range(NY):
                kept[k] = produce(k * NC + core)

    def far_copy(step):
        to = (y + step) % NY
        return remote(far_out.at[to], far_in.at[y], f_send.at[step], f_recv.at[step], r, to * NC + c)

    for step in range(1, NY):
        to = (y + step) % NY
        remote(near_in.at[to], near_in.at[to], n_send.at[to], n_recv.at[to], r, m).wait_recv()
        far_out[to] = (kept[to] + near_in[to].astype(F32)).astype(BF)
        far_copy(step).start()
    remote(near_in.at[y], near_in.at[y], n_send.at[y], n_recv.at[y], r, m).wait_recv()
    answer = kept[y] + near_in[y].astype(F32)
    for step in range(1, NY):
        origin = (y + NY - step) % NY
        remote(far_in.at[origin], far_in.at[origin], f_send.at[step], f_recv.at[step], r, m).wait_recv()
        answer = answer + far_in[origin].astype(F32)
    back_out[...] = answer.astype(BF).reshape(back_out.shape)

    def send_back(step, carry):
        to = (r + step) % count_req
        remote(back_out.at[to], back_in.at[r], b_send.at[step], b_recv.at[step], to, m).start()
        return carry

    lax.fori_loop(1, count_req, send_back, 0)
    back_in[r] = back_out[r]

    for step in range(1, count_mdl):
        origin = (m + count_mdl - step) % count_mdl
        remote(logits_in.at[origin], logits_in.at[origin], l_send.at[step], l_recv.at[step], r, m).wait_recv()
    both = logits_in[0]
    for k in range(1, count_mdl):
        both = both + logits_in[k]
    row_root = lax.rsqrt(both[:, count_req : count_req + 1] * (1.0 / width) + norm_epsilon)
    logits = both[:, 0:count_req] * row_root + router_bias[...]
    logits = jnp.where(hot > 0.5, logits, -jnp.inf)
    weight = jnp.exp(logits - jnp.max(logits, axis=1, keepdims=True))
    gates = weight / jnp.sum(weight, axis=1, keepdims=True)
    result = share_f32[...]
    biases = split3(gains[8 : 8 + count_req, :])
    gate_parts = split3(gates)
    for i in range(3):
        for j in range(3 - i):
            result = result + dot(gate_parts[i], biases[j])
    takers = [(take_rows * dot(piece, spread_t)).astype(BF) for piece in gate_parts]

    def take_back(step, carry):
        origin = (r + count_req - step) % count_req
        remote(back_in.at[origin], back_in.at[origin], b_send.at[step], b_recv.at[step], r, m).wait_recv()
        return carry

    lax.fori_loop(1, count_req, take_back, 0)
    returned = back_in[...].reshape(rows, share)
    for taker in takers:
        result = result + dot(taker, returned)
    out[...] = result.astype(BF)

    for step in range(1, NX):
        to = (x + step) % NX
        remote(att, heads.at[x], x_send.at[step], x_recv.at[step], to * NZ + z, m).wait_send()
    for step in range(NX):
        for j in range(per_group):

            @pl.when(jnp.logical_or(step > 0, per_group * x + j != m))
            def _():
                sum_copy(step, j).wait_send()

    def sent(step, carry):
        to = (r + step) % count_req
        remote(outgoing.at[to], gathered.at[m, r], d_send.at[step], d_recv.at[r], to, m).wait_send()
        remote(back_out.at[to], back_in.at[r], b_send.at[step], b_recv.at[step], to, m).wait_send()
        return carry

    lax.fori_loop(1, count_req, sent, 0)
    ring.finish()
    for way, dist, part in pair_plan:
        pair_copy(way, dist, part).wait_send()
    for k in range(NY):
        near_copy(k).wait_send()
    for step in range(1, NY):
        far_copy(step).wait_send()
    for step in range(1, count_mdl):
        to = (m + step) % count_mdl
        remote(logits_out, logits_in.at[m], l_send.at[step], l_recv.at[step], r, to).wait_send()


def experts(att, wo_all, hidden, obias, egain, router, router_bias, routes, routes_t, w1, b1, w2, rbias):
    tokens, width = hidden.shape
    count_req, count_mdl = NX * NZ, NY * NC
    share = width // count_mdl
    padded = -(-(share + 3) // 128) * 128
    rows = count_req * SLOTS
    columns = w1.shape[0]
    wide = -(-(columns + 1) // 128) * 128
    per_group = count_mdl // NX
    vmem = pl.BlockSpec(memory_space=pltpu.VMEM)
    hbm = pl.BlockSpec(memory_space=pl.ANY)
    dma = pltpu.SemaphoreType.DMA
    return pl.pallas_call(
        expert_kernel,
        name="experts",
        out_shape=jax.ShapeDtypeStruct((tokens, share), BF),
        in_specs=[vmem] * 9 + [hbm, vmem, hbm, vmem],
        out_specs=vmem,
        scratch_shapes=[
            pltpu.VMEM(w1.shape, BF),
            pltpu.VMEM(w2.shape, BF),
            pltpu.VMEM((NX,) + att.shape, BF),
            pltpu.VMEM((per_group, NX, tokens, share), BF),
            pltpu.VMEM((count_mdl, tokens, share), BF),
            pltpu.VMEM((tokens, padded), BF),
            pltpu.VMEM((count_req, SLOTS, padded), BF),
            pltpu.VMEM((count_mdl, count_req, SLOTS, padded), BF),
            pltpu.VMEM((rows, width), BF),
            pltpu.VMEM((rows, wide), F32),
            pltpu.VMEM((NY, rows, share), BF),
            pltpu.VMEM((NY, rows, share), BF),
            pltpu.VMEM((NY, rows, share), BF),
            pltpu.VMEM((NY, rows, share), BF),
            pltpu.VMEM((NY, rows, share), F32),
            pltpu.VMEM((count_req, SLOTS, share), BF),
            pltpu.VMEM((count_req, SLOTS, share), BF),
            pltpu.VMEM((tokens, 128), F32),
            pltpu.VMEM((count_mdl, tokens, 128), F32),
            pltpu.VMEM((tokens, share), F32),
            pltpu.VMEM((8 + 2 * count_req, share), F32),
            dma((NX,)), dma((NX,)),
            dma((NX * per_group,)), dma((count_mdl,)),
            dma((count_req,)), dma((count_req,)),
            *ring_sems(NY),
            dma((2 * (NY + 2),)), dma((2 * (NY + 2),)),
            dma((NY,)), dma((NY,)),
            dma((NY,)), dma((NY,)),
            dma((count_req,)), dma((count_req,)),
            dma((count_mdl,)), dma((count_mdl,)),
            dma((2,)),
        ],
        compiler_params=pltpu.CompilerParams(
            collective_id=2, has_side_effects=True, vmem_limit_bytes=VMEM_LIMIT
        ),
    )(att, wo_all, hidden, obias, egain, router, router_bias, routes, routes_t, w1, b1, w2, rbias)


def rotation_tables(lengths, repeat):
    half = HEAD_SIZE // 2
    exponent = jnp.arange(half, dtype=F32) * (2.0 / HEAD_SIZE)
    frequency = jnp.power(rope_theta, -exponent)
    angles = lengths.astype(F32)[:, None] * frequency[None, :]
    cosine, sine = jnp.cos(angles), jnp.sin(angles)
    return (
        jnp.concatenate([cosine, cosine] * repeat, axis=1),
        jnp.concatenate([-sine, sine] * repeat, axis=1),
    )


def shards(
    hidden_state,
    cached_length_list,
    page_table,
    paged_cache_store,
    attention_gain,
    qkv_weight,
    qkv_bias,
    sink_logit_values,
    output_weight,
    output_bias,
    expert_gain,
    router_weight,
    router_bias,
    expert_routes,
    expand_weight,
    expand_bias,
    reduce_weight,
    reduce_bias,
):
    projected, wo_all = project(
        hidden_state, attention_gain[None], qkv_weight, output_weight.T, qkv_bias[None]
    )
    pool = paged_cache_store.shape[0]
    local_table = jnp.clip(page_table - lax.axis_index("req") * pool, 0, pool - 1)
    cosines, sines = rotation_tables(cached_length_list, 2)
    attended = attend(
        cached_length_list, local_table, projected, cosines, sines, sink_logit_values[:, None], paged_cache_store
    )
    return experts(
        attended,
        wo_all,
        hidden_state,
        output_bias[None],
        expert_gain[None],
        router_weight.T,
        router_bias[None],
        expert_routes,
        expert_routes.T,
        expand_weight[0].T,
        expand_bias,
        reduce_weight[0],
        reduce_bias,
    )


def solution(mesh):
    in_specs = (
        P("req", None),
        P("req"),
        P("req", None),
        P("req", None, "mdl"),
        P(),
        P("req", "mdl"),
        P("mdl"),
        P("mdl"),
        P("mdl", "req"),
        P(),
        P(),
        P(),
        P(),
        P("req", None),
        P("req", None, "mdl"),
        P("req", "mdl"),
        P("req", "mdl", None),
        P(),
    )
    out_specs = P("req", "mdl")
    return jax.shard_map(shards, mesh=mesh, in_specs=in_specs, out_specs=out_specs, check_vma=False)
```

```python
import functools
import math

import jax
import jax.numpy as jnp
from jax import lax
from jax.experimental import pallas as pl
from jax.experimental.pallas import tpu as pltpu
from jax.sharding import PartitionSpec as P

HEAD_SIZE = 64
PAGE_POSITIONS = 128
SHORT_MAX = 256
QUERY_PER_KEY = 8
SHORT_PAGES = 2
SLOTS = 8

NX, NZ, NY, NC = 4, 8, 4, 2

norm_epsilon = 1e-05
rope_theta = 150000.0
swiglu_limit = 7.0
swiglu_alpha = 1.702

BF = jnp.bfloat16
F32 = jnp.float32
VMEM_LIMIT = 58 * 2**20
LOWEST = -1e30
MESH = pl.DeviceIdType.MESH


def place():
    r = lax.axis_index("req")
    m = lax.axis_index("mdl")
    return r, m, r // NZ, r % NZ, m // NC, m % NC


def device(r, m):
    return {"req": r, "mdl": m}


def dot(a, b):
    return jnp.dot(a, b, preferred_element_type=F32)


def dot_nt(a, b):
    return lax.dot_general(a, b, (((1,), (1,)), ((), ())), preferred_element_type=F32)


def split3(value):
    high = value.astype(BF)
    rest = value - high.astype(F32)
    middle = rest.astype(BF)
    low = (rest - middle.astype(F32)).astype(BF)
    return high, middle, low


class Ring:
    def __init__(self, size, me, ref_of, send, recv, target):
        self.size, self.me, self.ref_of = size, me, ref_of
        self.send, self.recv, self.target = send, recv, target
        self.half = size // 2
        self.plan = [
            (way, dist, part)
            for dist in range(1, self.half + 1)
            for part in range(2)
            for way in range(2)
            if self.exists(way, dist, part)
        ]

    def exists(self, way, dist, part):
        return dist < self.half or (dist == self.half and part == way)

    def index(self, way, dist, part):
        return (way * self.half + dist - 1) * 2 + part

    def origin(self, way, dist):
        return (self.me + (dist if way else self.size - dist)) % self.size

    def copy(self, way, dist, part):
        ref = self.ref_of(self.origin(way, dist - 1), part)
        i = self.index(way, dist, part)
        to = (self.me + (self.size - 1 if way else 1)) % self.size
        return pltpu.make_async_remote_copy(
            src_ref=ref,
            dst_ref=ref,
            send_sem=self.send.at[i],
            recv_sem=self.recv.at[i],
            device_id=self.target(to),
            device_id_type=MESH,
        )

    def arrive(self, way, dist, part):
        ref = self.ref_of(self.origin(way, dist), part)
        i = self.index(way, dist, part)
        pltpu.make_async_remote_copy(
            src_ref=ref,
            dst_ref=ref,
            send_sem=self.send.at[i],
            recv_sem=self.recv.at[i],
            device_id=self.target(self.me),
            device_id_type=MESH,
        ).wait_recv()

    def begin(self, part):
        for way in range(2):
            if self.exists(way, 1, part):
                self.copy(way, 1, part).start()

    def step(self, way, dist, part):
        self.arrive(way, dist, part)
        if self.exists(way, dist + 1, part):
            self.copy(way, dist + 1, part).start()

    def finish(self):
        for way, dist, part in self.plan:
            self.copy(way, dist, part).wait_send()


def remote(src, dst, send, recv, r, m):
    return pltpu.make_async_remote_copy(
        src_ref=src,
        dst_ref=dst,
        send_sem=send,
        recv_sem=recv,
        device_id=device(r, m),
        device_id_type=MESH,
    )


def ring_sems(size):
    return [pltpu.SemaphoreType.DMA((2 * size,)), pltpu.SemaphoreType.DMA((2 * size,))]


def lane_cut(width):
    tiles = width // 128
    return 128 * ((tiles + 1) // 2) if tiles > 1 else 0


def project_kernel(
    hidden, gain, wqkv, wo, bias,
    proj, wo_out,
    gathered, wo_all, parcels, rows, blocks, total, sums, sums_in,
    ring_send, ring_recv, wo_send, wo_recv, x_send, x_recv, s_send, s_recv, local,
):
    r, m, x, z, y, c = place()
    tokens, width = hidden.shape
    group = width // NX
    block = group // NZ

    load_q = pltpu.make_async_copy(wqkv, gathered.at[z], local.at[0])
    load_o = pltpu.make_async_copy(wo, wo_all.at[z], local.at[1])
    load_q.start()
    load_o.start()

    barrier = pltpu.get_barrier_semaphore()
    for step in (1, NZ - 1):
        pl.semaphore_signal(barrier, inc=1, device_id=device(x * NZ + (z + step) % NZ, m), device_id_type=MESH)
    for step in range(1, NX):
        pl.semaphore_signal(barrier, inc=1, device_id=device((x + step) % NX * NZ + z, m), device_id_type=MESH)
    load_q.wait()
    pl.semaphore_wait(barrier, NX + 1)

    cut_q, cut_o = lane_cut(wqkv.shape[1]), lane_cut(wo.shape[1])

    def part_of(buffer, cut):
        full = buffer.shape[-1]

        def ref_of(origin, part):
            return buffer.at[origin, :, pl.ds(0, cut) if part == 0 else pl.ds(cut, full - cut)]

        return ref_of

    def at_z(to):
        return device(x * NZ + to, m)

    ring = Ring(NZ, z, part_of(gathered, cut_q), ring_send, ring_recv, at_z)
    ring_o = Ring(NZ, z, part_of(wo_all, cut_o), wo_send, wo_recv, at_z)
    for part in range(2):
        ring.begin(part)

    value = hidden[...].astype(F32)
    scale = lax.rsqrt(jnp.mean(value * value, axis=-1, keepdims=True) + norm_epsilon)
    normed = (value * scale * gain[...]).astype(BF)
    for k in range(NX):
        parcels[k] = normed[:, group * k : group * k + group]

    def x_copy(src, dst, send, recv, step):
        to = (x + step) % NX
        return remote(src.at[to], dst.at[x], send.at[step], recv.at[step], to * NZ + z, m)

    def x_arrive(dst, send, recv, step):
        origin = (x + NX - step) % NX
        remote(dst.at[origin], dst.at[origin], send.at[step], recv.at[step], r, m).wait_recv()

    for step in range(1, NX):
        x_copy(parcels, rows, x_send, x_recv, step).start()
    rows[x] = parcels[x]

    for step in range(1, NX):
        x_arrive(rows, x_send, x_recv, step)
    for k in range(NZ):
        for j in range(NX):
            blocks[k, j * tokens : (j + 1) * tokens] = rows[j, :, block * k : block * k + block]

    def add(origin, first):
        product = dot(blocks[origin], gathered[origin])
        for j in range(NX):
            piece = product[j * tokens : (j + 1) * tokens]
            total[j] = piece if first else total[j] + piece

    add(z, True)
    for dist in range(1, ring.half + 1):
        for way, d, part in ring.plan:
            if d == dist:
                ring.step(way, d, part)
        if dist == ring.half - 1 or ring.half == 1:
            load_o.wait()
            for part in range(2):
                ring_o.begin(part)
        add(ring.origin(0, dist), False)
        if dist < ring.half:
            add(ring.origin(1, dist), False)

    for j in range(NX):
        sums[j] = total[j].astype(BF)
    for step in range(1, NX):
        x_copy(sums, sums_in, s_send, s_recv, step).start()
    for way, dist, part in ring_o.plan:
        ring_o.step(way, dist, part)
    result = total[x] + bias[...]
    for step in range(1, NX):
        x_arrive(sums_in, s_send, s_recv, step)
        result = result + sums_in[(x + NX - step) % NX].astype(F32)
    proj[...] = result
    for k in range(NZ):
        wo_out[k] = wo_all[k]

    ring.finish()
    ring_o.finish()
    for step in range(1, NX):
        x_copy(parcels, rows, x_send, x_recv, step).wait_send()
        x_copy(sums, sums_in, s_send, s_recv, step).wait_send()


def project(hidden, gain, wqkv, wo, bias):
    tokens, width = hidden.shape
    group = width // NX
    block, cols = wqkv.shape
    out_rows = wo.shape[1]
    vmem = pl.BlockSpec(memory_space=pltpu.VMEM)
    hbm = pl.BlockSpec(memory_space=pl.ANY)
    return pl.pallas_call(
        project_kernel,
        name="project",
        out_shape=(
            jax.ShapeDtypeStruct((tokens, cols), F32),
            jax.ShapeDtypeStruct((NZ, block, out_rows), BF),
        ),
        in_specs=[vmem, vmem, hbm, hbm, vmem],
        out_specs=(vmem, vmem),
        scratch_shapes=[
            pltpu.VMEM((NZ, block, cols), BF),
            pltpu.VMEM((NZ, block, out_rows), BF),
            pltpu.VMEM((NX, tokens, group), BF),
            pltpu.VMEM((NX, tokens, group), BF),
            pltpu.VMEM((NZ, NX * tokens, block), BF),
            pltpu.VMEM((NX, tokens, cols), F32),
            pltpu.VMEM((NX, tokens, cols), BF),
            pltpu.VMEM((NX, tokens, cols), BF),
            *ring_sems(NZ),
            *ring_sems(NZ),
            *[pltpu.SemaphoreType.DMA((NX,))] * 4,
            pltpu.SemaphoreType.DMA((2,)),
        ],
        compiler_params=pltpu.CompilerParams(
            collective_id=1, has_side_effects=True, vmem_limit_bytes=VMEM_LIMIT
        ),
    )(hidden, gain, wqkv, wo, bias)


def find_long(lengths, count, most_long, rank, at_long):
    def see(i, carry):
        seen, places = carry
        rank[i] = jnp.minimum(seen, most_long - 1)
        seen = seen + (lengths[i] > SHORT_MAX).astype(jnp.int32)
        return seen, tuple(p + (seen <= j).astype(jnp.int32) for j, p in enumerate(places))

    zero = jnp.int32(0)
    _, places = lax.fori_loop(0, count, see, (zero, (zero,) * most_long))
    for j in range(most_long):
        at_long[j] = jnp.minimum(places[j], count - 1)


def attend_kernel(
    lengths, table, proj, cosines, sines, sinks, cache,
    out,
    pool, rank, at_long, scores, far_scores, queries, owns, tops, bottoms, mixed,
    far_top, far_bottom, far_mixed, load,
):
    r = lax.axis_index("req")
    load_pool = pltpu.make_async_copy(cache, pool, load.at[0])
    load_pool.start()
    count = proj.shape[0]
    heads = QUERY_PER_KEY
    most_long = far_scores.shape[0]
    find_long(lengths, count, most_long, rank, at_long)
    pages = table.shape[0]
    channels = pool.shape[2]
    score_scale = 1.0 / math.sqrt(HEAD_SIZE)
    base = r * pool.shape[0]

    value = proj[...]
    lanes = lax.broadcasted_iota(jnp.int32, value.shape, 1)
    width = value.shape[1]
    first = (lanes % HEAD_SIZE) < HEAD_SIZE // 2
    partner = jnp.where(
        first,
        pltpu.roll(value, width - HEAD_SIZE // 2, axis=1),
        pltpu.roll(value, HEAD_SIZE // 2, axis=1),
    )
    repeat = width // cosines.shape[1]
    turned = value * jnp.concatenate([cosines[...]] * repeat, axis=1) + partner * jnp.concatenate(
        [sines[...]] * repeat, axis=1
    )
    key_at = heads * HEAD_SIZE
    rounded = jnp.where(lanes < key_at + HEAD_SIZE, turned, value).astype(BF).astype(F32)
    new_key = rounded[:, key_at : key_at + HEAD_SIZE]
    new_value = rounded[:, key_at + HEAD_SIZE :]
    queries[...] = jnp.zeros_like(queries)
    for h in range(heads):
        head = rounded[:, h * HEAD_SIZE : (h + 1) * HEAD_SIZE]
        queries[:, h, 0:HEAD_SIZE] = head
        own = jnp.sum(head * new_key, axis=1, keepdims=True) * score_scale
        owns[:, h, :] = jnp.broadcast_to(own, (count, channels))
    load_pool.wait()

    def entries(i, start, stop):
        return jnp.concatenate(
            [pool[jnp.clip(table[p, i] - base, 0, pool.shape[0] - 1)] for p in range(start, stop)], axis=0
        )

    def masked(raw, i, start):
        positions = lax.broadcasted_iota(jnp.int32, raw.shape, 1) + start
        return jnp.where(positions < lengths[i], raw * score_scale, LOWEST)

    at_once = 8 if count % 8 == 0 else 1

    def score(g, carry):
        for u in range(at_once):
            i = g * at_once + u
            scores[i] = masked(dot_nt(queries[i].astype(BF), entries(i, 0, SHORT_PAGES)), i, 0)
        return carry

    lax.fori_loop(0, count // at_once, score, 0)

    def far_score(j, carry):
        i = at_long[j]
        far_scores[j] = masked(dot_nt(queries[i].astype(BF), entries(i, SHORT_PAGES, pages)), i, SHORT_MAX)
        return carry

    lax.fori_loop(0, most_long, far_score, 0)

    def weigh(held, tops, bottoms):
        raw = held[...]
        top = jnp.max(raw, axis=2, keepdims=True)
        weight = jnp.exp(raw - top)
        held[...] = weight
        tops[...] = jnp.broadcast_to(top, tops.shape)
        bottoms[...] = jnp.broadcast_to(jnp.sum(weight, axis=2, keepdims=True), bottoms.shape)

    weigh(scores, tops, bottoms)
    weigh(far_scores, far_top, far_bottom)

    def mix(g, carry):
        for u in range(at_once):
            i = g * at_once + u
            mixed[i] = dot(scores[i].astype(BF), entries(i, 0, SHORT_PAGES))
        return carry

    lax.fori_loop(0, count // at_once, mix, 0)

    def far_mix(j, carry):
        far_mixed[j] = dot(far_scores[j].astype(BF), entries(at_long[j], SHORT_PAGES, pages))
        return carry

    lax.fori_loop(0, most_long, far_mix, 0)

    sink_rows = lax.broadcasted_iota(jnp.int32, (heads, channels), 0)
    sink = jnp.zeros((heads, channels), F32)
    for h in range(heads):
        sink = jnp.where(sink_rows == h, sinks[h], sink)

    def join(g, carry):
        for u in range(at_once):
            i = g * at_once + u
            k = rank[i]
            is_long = jnp.full((heads, channels), lengths[i], jnp.int32) > SHORT_MAX
            far = jnp.where(is_long, far_top[k], LOWEST)
            own = owns[i]
            near = tops[i]
            top = jnp.maximum(jnp.maximum(near, far), jnp.maximum(own, sink))
            near_scale = jnp.exp(near - top)
            far_scale = jnp.exp(far - top)
            own_weight = jnp.exp(own - top)
            bottom = bottoms[i] * near_scale + own_weight + jnp.exp(sink - top)
            bottom = bottom + jnp.where(is_long, far_bottom[k] * far_scale, 0.0)
            both = mixed[i] * near_scale + jnp.where(is_long, far_mixed[k] * far_scale, 0.0)
            mixed[i] = both / bottom
            owns[i] = own_weight / bottom
        return carry

    lax.fori_loop(0, count // at_once, join, 0)
    for h in range(heads):
        head = mixed[:, h, HEAD_SIZE:] + owns[:, h, 0:1] * new_value
        out[:, h * HEAD_SIZE : (h + 1) * HEAD_SIZE] = head.astype(BF)


def attend(lengths, table, proj, cosines, sines, sinks, cache):
    tokens = proj.shape[0]
    channels = cache.shape[2]
    pages = table.shape[0]
    most_long = tokens // 4
    vmem = pl.BlockSpec(memory_space=pltpu.VMEM)
    smem = pl.BlockSpec(memory_space=pltpu.SMEM)
    per_head = pltpu.VMEM((tokens, QUERY_PER_KEY, channels), F32)
    per_long = pltpu.VMEM((most_long, QUERY_PER_KEY, channels), F32)
    return pl.pallas_call(
        attend_kernel,
        name="attend",
        out_shape=jax.ShapeDtypeStruct((tokens, QUERY_PER_KEY * HEAD_SIZE), BF),
        in_specs=[smem, smem, vmem, vmem, vmem, smem, pl.BlockSpec(memory_space=pl.ANY)],
        out_specs=vmem,
        scratch_shapes=[
            pltpu.VMEM(cache.shape, BF),
            pltpu.SMEM((tokens,), jnp.int32),
            pltpu.SMEM((most_long,), jnp.int32),
            pltpu.VMEM((tokens, QUERY_PER_KEY, SHORT_PAGES * PAGE_POSITIONS), F32),
            pltpu.VMEM((most_long, QUERY_PER_KEY, (pages - SHORT_PAGES) * PAGE_POSITIONS), F32),
            *[per_head] * 5,
            *[per_long] * 3,
            pltpu.SemaphoreType.DMA((1,)),
        ],
        compiler_params=pltpu.CompilerParams(vmem_limit_bytes=VMEM_LIMIT),
    )(lengths, table, proj, cosines, sines, sinks, cache)


def expert_kernel(
    att, wo_all, hidden, obias, egain, router, router_bias, routes_t, w1_hbm, b1, w2_hbm, rbias,
    out,
    w1, w2, heads, halves, summed, mine, outgoing, gathered, full, pre, near_out, near_in, far_out, far_in,
    kept, back_out, back_in, logits_out, logits_in, share_f32, gains,
    x_send, x_recv, s_send, s_recv, d_send, d_recv, ring_send, ring_recv, p_send, p_recv,
    n_send, n_recv, f_send, f_recv, b_send, b_recv, l_send, l_recv, local,
):
    r, m, x, z, y, c = place()
    tokens, width = hidden.shape
    count_req, count_mdl = NX * NZ, NY * NC
    share = width // count_mdl
    block = width // count_req
    padded = outgoing.shape[2]
    rows = count_req * SLOTS
    per_group = NZ * block // share

    load1 = pltpu.make_async_copy(w1_hbm, w1, local.at[0])
    load2 = pltpu.make_async_copy(w2_hbm, w2, local.at[1])
    load1.start()
    load2.start()

    barrier = pltpu.get_barrier_semaphore()

    def greet(to_r, to_m):
        pl.semaphore_signal(barrier, inc=1, device_id=device(to_r, to_m), device_id_type=MESH)

    def greet_req(step, carry):
        greet((r + step) % count_req, m)
        return carry

    lax.fori_loop(1, count_req, greet_req, 0)
    for step in range(1, count_mdl):
        greet(r, (m + step) % count_mdl)
    diagonal = x == y
    for step in range(NX):
        for j in range(per_group):
            not_me = jnp.logical_or(step > 0, per_group * x + j != m)

            @pl.when(not_me)
            def _():
                greet((x + step) % NX * NZ + z, per_group * x + j)

    for j in range(count_mdl):

        @pl.when(jnp.logical_not(jnp.logical_and(diagonal, m == j)))
        def _():
            greet(y * NZ + z, j)

    pl.semaphore_wait(
        barrier,
        (count_req - 1) + (count_mdl - 1) + NX * per_group + count_mdl - 2 * diagonal.astype(jnp.int32),
    )

    for step in range(1, NX):
        to = (x + step) % NX
        remote(att, heads.at[x], x_send.at[step], x_recv.at[step], to * NZ + z, m).start()
    heads[x] = att[...]

    for k in range(count_mdl):

        @pl.when(m == k)
        def _():
            at = slice(share * k, share * k + share)
            share_f32[...] = hidden[:, at].astype(F32) + obias[:, at]
            gains[0:1, :] = egain[:, at]
            gains[8 : 8 + count_req, :] = rbias[:, at]
            gains[8 + count_req : 8 + 2 * count_req, :] = router[:, at].astype(F32)

    names = lax.broadcasted_iota(jnp.int32, (count_req, tokens), 0)
    hot_t = jnp.zeros((count_req, tokens), F32)
    for k in range(routes_t.shape[0]):
        hot_t = hot_t + (routes_t[k : k + 1, :] == names).astype(F32)
    same = lax.broadcasted_iota(jnp.int32, (tokens, tokens), 0) == lax.broadcasted_iota(
        jnp.int32, (tokens, tokens), 1
    )
    hot = dot_nt(same.astype(BF), hot_t.astype(BF))
    before = lax.broadcasted_iota(jnp.int32, (tokens, tokens), 0) < lax.broadcasted_iota(
        jnp.int32, (tokens, tokens), 1
    )
    rank_t = dot(hot_t.astype(BF), before.astype(BF))
    after = lax.broadcasted_iota(jnp.int32, (tokens, tokens), 0) > lax.broadcasted_iota(
        jnp.int32, (tokens, tokens), 1
    )
    rank = dot(after.astype(BF), hot.astype(BF))
    spread = (
        lax.broadcasted_iota(jnp.int32, (rows, count_req), 0) // SLOTS
        == lax.broadcasted_iota(jnp.int32, (rows, count_req), 1)
    ).astype(BF)
    spread_t = (
        lax.broadcasted_iota(jnp.int32, (count_req, rows), 1) // SLOTS
        == lax.broadcasted_iota(jnp.int32, (count_req, rows), 0)
    ).astype(BF)
    slot = (lax.broadcasted_iota(jnp.int32, (rows, tokens), 0) % SLOTS).astype(F32)
    place_rows = jnp.where(
        jnp.logical_and(dot(spread, hot_t.astype(BF)) > 0.5, dot(spread, rank_t.astype(BF)) == slot), 1.0, 0.0
    ).astype(BF)
    slot_t = (lax.broadcasted_iota(jnp.int32, (tokens, rows), 1) % SLOTS).astype(F32)
    take_rows = jnp.where(
        jnp.logical_and(dot(hot.astype(BF), spread_t) > 0.5, dot(rank.astype(BF), spread_t) == slot_t), 1.0, 0.0
    )

    for step in range(1, NX):
        origin = (x + NX - step) % NX
        remote(heads.at[origin], heads.at[origin], x_send.at[step], x_recv.at[step], r, m).wait_recv()

    stacked = jnp.concatenate([heads[j] for j in range(NX)], axis=0)
    per_share = share // block
    for k in range(NZ):
        product = dot_nt(stacked, wo_all[k]).astype(BF)
        for j in range(NX):
            halves[k // per_share, j, :, block * (k % per_share) : block * (k % per_share) + block] = product[
                j * tokens : (j + 1) * tokens
            ]

    def sum_copy(step, j):
        to = (x + step) % NX
        i = step * per_group + j
        return remote(
            halves.at[j, to], summed.at[m], s_send.at[i], s_recv.at[m], to * NZ + z, per_group * x + j
        )

    for step in range(NX):
        for j in range(per_group):

            @pl.when(jnp.logical_or(step > 0, per_group * x + j != m))
            def _():
                sum_copy(step, j).start()

    @pl.when(diagonal)
    def _():
        summed[m] = halves[m % per_group, x]

    residual = share_f32[...]
    for j in range(count_mdl):

        @pl.when(jnp.logical_not(jnp.logical_and(diagonal, m == j)))
        def _():
            remote(summed.at[j], summed.at[j], s_send.at[0], s_recv.at[j], r, m).wait_recv()

    total = summed[0].astype(F32)
    for j in range(1, count_mdl):
        total = total + summed[j].astype(F32)
    residual = (residual + total).astype(BF).astype(F32)
    share_f32[...] = residual
    squares = jnp.sum(residual * residual, axis=1, keepdims=True)
    scaled = (residual * gains[0:1, :]).astype(BF)
    mine[...] = jnp.zeros_like(mine)
    mine[:, 0:share] = scaled
    for k, piece in enumerate(split3(squares)):
        mine[:, share + k : share + k + 1] = piece

    outgoing[...] = dot(place_rows, mine[...]).astype(BF).reshape(outgoing.shape)

    def send_row(step, carry):
        to = (r + step) % count_req
        remote(outgoing.at[to], gathered.at[m, r], d_send.at[step], d_recv.at[r], to, m).start()
        return carry

    lax.fori_loop(1, count_req, send_row, 0)
    gathered[m, r] = outgoing[r]

    routing = gains[8 + count_req : 8 + 2 * count_req, :].astype(BF)
    logits_out[...] = jnp.zeros_like(logits_out)
    logits_out[:, 0:count_req] = dot_nt(scaled, routing)
    logits_out[:, count_req : count_req + 1] = squares
    for step in range(1, count_mdl):
        to = (m + step) % count_mdl
        remote(logits_out, logits_in.at[m], l_send.at[step], l_recv.at[step], r, to).start()
    logits_in[m] = logits_out[...]

    part_rows = count_req // 2

    def part_ref(origin, part):
        return gathered.at[origin * NC + c, pl.ds(part * part_rows, part_rows)]

    def at_y(to):
        return device(r, to * NC + c)

    ring = Ring(NY, y, part_ref, ring_send, ring_recv, at_y)

    def pair_index(way, dist):
        return way * ring.half + dist

    def pair_copy(way, dist, part):
        origin = ring.origin(way, dist)
        ref = part_ref(origin, part)
        i = pair_index(way, dist) * 2 + part
        return remote(ref, ref, p_send.at[i], p_recv.at[i], r, y * NC + 1 - c)

    def pair_arrive(way, dist, part):
        ref = gathered.at[ring.origin(way, dist) * NC + 1 - c, pl.ds(part * part_rows, part_rows)]
        i = pair_index(way, dist) * 2 + part
        remote(ref, ref, p_send.at[i], p_recv.at[i], r, m).wait_recv()

    for part in range(2):

        def take(origin, carry):
            @pl.when(origin != r)
            def _():
                remote(gathered.at[m, origin], gathered.at[m, origin], d_send.at[0], d_recv.at[origin], r, m).wait_recv()

            return carry

        lax.fori_loop(part * part_rows, (part + 1) * part_rows, take, 0)
        ring.begin(part)
        pair_copy(0, 0, part).start()

    for way, dist, part in ring.plan:
        ring.step(way, dist, part)
        pair_copy(way, dist, part).start()
    pair_plan = [(0, 0, 0), (0, 0, 1)] + ring.plan
    for way, dist, part in pair_plan:
        pair_arrive(way, dist, part)

    load1.wait()
    load2.wait()
    square_sum = jnp.zeros((rows, 1), F32)
    for k in range(count_mdl):
        piece = gathered[k].reshape(rows, padded)
        full[:, share * k : share * k + share] = piece[:, 0:share]
        for j in range(3):
            square_sum = square_sum + piece[:, share + j : share + j + 1].astype(F32)
    root = lax.rsqrt(square_sum * (1.0 / width) + norm_epsilon)
    columns = w1.shape[0]
    pre[...] = jnp.zeros_like(pre)
    pre[:, 0:columns] = dot_nt(full[...], w1[...]) * root + b1[...]
    raw = pre[...]
    up = jnp.clip(pltpu.roll(raw, raw.shape[1] - 1, axis=1), -swiglu_limit, swiglu_limit)
    gate = jnp.minimum(raw, swiglu_limit)
    act = (gate * jax.nn.sigmoid(swiglu_alpha * gate) * (up + 1.0)).astype(BF)
    hidden_units = columns // 2
    pick = (
        lax.broadcasted_iota(jnp.int32, (raw.shape[1], hidden_units), 0)
        == 2 * lax.broadcasted_iota(jnp.int32, (raw.shape[1], hidden_units), 1)
    ).astype(BF)
    act = dot(act, pick).astype(BF)

    def produce(k):
        return dot(act, w2[:, share * k : share * k + share])

    def near_copy(k):
        return remote(near_out.at[k], near_in.at[k], n_send.at[k], n_recv.at[k], r, y * NC + 1 - c)

    for core in range(NC):

        @pl.when(c == core)
        def _():
            for k in range(NY):
                near_out[k] = produce(k * NC + 1 - core).astype(BF)
                near_copy(k).start()
            for k in range(NY):
                kept[k] = produce(k * NC + core)

    def far_copy(step):
        to = (y + step) % NY
        return remote(far_out.at[to], far_in.at[y], f_send.at[step], f_recv.at[step], r, to * NC + c)

    for step in range(1, NY):
        to = (y + step) % NY
        remote(near_in.at[to], near_in.at[to], n_send.at[to], n_recv.at[to], r, m).wait_recv()
        far_out[to] = (kept[to] + near_in[to].astype(F32)).astype(BF)
        far_copy(step).start()
    remote(near_in.at[y], near_in.at[y], n_send.at[y], n_recv.at[y], r, m).wait_recv()
    answer = kept[y] + near_in[y].astype(F32)
    for step in range(1, NY):
        origin = (y + NY - step) % NY
        remote(far_in.at[origin], far_in.at[origin], f_send.at[step], f_recv.at[step], r, m).wait_recv()
        answer = answer + far_in[origin].astype(F32)
    back_out[...] = answer.astype(BF).reshape(back_out.shape)

    def send_back(step, carry):
        to = (r + step) % count_req
        remote(back_out.at[to], back_in.at[r], b_send.at[step], b_recv.at[step], to, m).start()
        return carry

    lax.fori_loop(1, count_req, send_back, 0)
    back_in[r] = back_out[r]

    for step in range(1, count_mdl):
        origin = (m + count_mdl - step) % count_mdl
        remote(logits_in.at[origin], logits_in.at[origin], l_send.at[step], l_recv.at[step], r, m).wait_recv()
    both = logits_in[0]
    for k in range(1, count_mdl):
        both = both + logits_in[k]
    row_root = lax.rsqrt(both[:, count_req : count_req + 1] * (1.0 / width) + norm_epsilon)
    logits = both[:, 0:count_req] * row_root + router_bias[...]
    logits = jnp.where(hot > 0.5, logits, -jnp.inf)
    weight = jnp.exp(logits - jnp.max(logits, axis=1, keepdims=True))
    gates = weight / jnp.sum(weight, axis=1, keepdims=True)
    result = share_f32[...]
    biases = split3(gains[8 : 8 + count_req, :])
    gate_parts = split3(gates)
    for i in range(3):
        for j in range(3 - i):
            result = result + dot(gate_parts[i], biases[j])
    takers = [(take_rows * dot(piece, spread_t)).astype(BF) for piece in gate_parts]

    def take_back(step, carry):
        origin = (r + count_req - step) % count_req
        remote(back_in.at[origin], back_in.at[origin], b_send.at[step], b_recv.at[step], r, m).wait_recv()
        return carry

    lax.fori_loop(1, count_req, take_back, 0)
    returned = back_in[...].reshape(rows, share)
    for taker in takers:
        result = result + dot(taker, returned)
    out[...] = result.astype(BF)

    for step in range(1, NX):
        to = (x + step) % NX
        remote(att, heads.at[x], x_send.at[step], x_recv.at[step], to * NZ + z, m).wait_send()
    for step in range(NX):
        for j in range(per_group):

            @pl.when(jnp.logical_or(step > 0, per_group * x + j != m))
            def _():
                sum_copy(step, j).wait_send()

    def sent(step, carry):
        to = (r + step) % count_req
        remote(outgoing.at[to], gathered.at[m, r], d_send.at[step], d_recv.at[r], to, m).wait_send()
        remote(back_out.at[to], back_in.at[r], b_send.at[step], b_recv.at[step], to, m).wait_send()
        return carry

    lax.fori_loop(1, count_req, sent, 0)
    ring.finish()
    for way, dist, part in pair_plan:
        pair_copy(way, dist, part).wait_send()
    for k in range(NY):
        near_copy(k).wait_send()
    for step in range(1, NY):
        far_copy(step).wait_send()
    for step in range(1, count_mdl):
        to = (m + step) % count_mdl
        remote(logits_out, logits_in.at[m], l_send.at[step], l_recv.at[step], r, to).wait_send()


def experts(att, wo_all, hidden, obias, egain, router, router_bias, routes_t, w1, b1, w2, rbias):
    tokens, width = hidden.shape
    count_req, count_mdl = NX * NZ, NY * NC
    share = width // count_mdl
    padded = -(-(share + 3) // 128) * 128
    rows = count_req * SLOTS
    columns = w1.shape[0]
    wide = -(-(columns + 1) // 128) * 128
    per_group = count_mdl // NX
    vmem = pl.BlockSpec(memory_space=pltpu.VMEM)
    hbm = pl.BlockSpec(memory_space=pl.ANY)
    dma = pltpu.SemaphoreType.DMA
    return pl.pallas_call(
        expert_kernel,
        name="experts",
        out_shape=jax.ShapeDtypeStruct((tokens, share), BF),
        in_specs=[vmem] * 8 + [hbm, vmem, hbm, vmem],
        out_specs=vmem,
        scratch_shapes=[
            pltpu.VMEM(w1.shape, BF),
            pltpu.VMEM(w2.shape, BF),
            pltpu.VMEM((NX,) + att.shape, BF),
            pltpu.VMEM((per_group, NX, tokens, share), BF),
            pltpu.VMEM((count_mdl, tokens, share), BF),
            pltpu.VMEM((tokens, padded), BF),
            pltpu.VMEM((count_req, SLOTS, padded), BF),
            pltpu.VMEM((count_mdl, count_req, SLOTS, padded), BF),
            pltpu.VMEM((rows, width), BF),
            pltpu.VMEM((rows, wide), F32),
            pltpu.VMEM((NY, rows, share), BF),
            pltpu.VMEM((NY, rows, share), BF),
            pltpu.VMEM((NY, rows, share), BF),
            pltpu.VMEM((NY, rows, share), BF),
            pltpu.VMEM((NY, rows, share), F32),
            pltpu.VMEM((count_req, SLOTS, share), BF),
            pltpu.VMEM((count_req, SLOTS, share), BF),
            pltpu.VMEM((tokens, 128), F32),
            pltpu.VMEM((count_mdl, tokens, 128), F32),
            pltpu.VMEM((tokens, share), F32),
            pltpu.VMEM((8 + 2 * count_req, share), F32),
            dma((NX,)), dma((NX,)),
            dma((NX * per_group,)), dma((count_mdl,)),
            dma((count_req,)), dma((count_req,)),
            *ring_sems(NY),
            dma((2 * (NY + 2),)), dma((2 * (NY + 2),)),
            dma((NY,)), dma((NY,)),
            dma((NY,)), dma((NY,)),
            dma((count_req,)), dma((count_req,)),
            dma((count_mdl,)), dma((count_mdl,)),
            dma((2,)),
        ],
        compiler_params=pltpu.CompilerParams(
            collective_id=2, has_side_effects=True, vmem_limit_bytes=VMEM_LIMIT
        ),
    )(att, wo_all, hidden, obias, egain, router, router_bias, routes_t, w1, b1, w2, rbias)


def rotation_tables(lengths, repeat):
    half = HEAD_SIZE // 2
    exponent = jnp.arange(half, dtype=F32) * (2.0 / HEAD_SIZE)
    frequency = jnp.power(rope_theta, -exponent)
    angles = lengths.astype(F32)[:, None] * frequency[None, :]
    cosine, sine = jnp.cos(angles), jnp.sin(angles)
    return (
        jnp.concatenate([cosine, cosine] * repeat, axis=1),
        jnp.concatenate([-sine, sine] * repeat, axis=1),
    )


def shards(
    hidden_state,
    cached_length_list,
    page_table,
    paged_cache_store,
    attention_gain,
    qkv_weight,
    qkv_bias,
    sink_logit_values,
    output_weight,
    output_bias,
    expert_gain,
    router_weight,
    router_bias,
    expert_routes,
    expand_weight,
    expand_bias,
    reduce_weight,
    reduce_bias,
):
    projected, wo_all = project(
        hidden_state, attention_gain[None], qkv_weight, output_weight.T, qkv_bias[None]
    )
    cosines, sines = rotation_tables(cached_length_list, 2)
    attended = attend(
        cached_length_list, page_table.T, projected, cosines, sines, sink_logit_values, paged_cache_store
    )
    return experts(
        attended,
        wo_all,
        hidden_state,
        output_bias[None],
        expert_gain[None],
        router_weight.T,
        router_bias[None],
        expert_routes.T,
        expand_weight[0].T,
        expand_bias,
        reduce_weight[0],
        reduce_bias,
    )


def solution(mesh):
    in_specs = (
        P("req", None),
        P("req"),
        P("req", None),
        P("req", None, "mdl"),
        P(),
        P("req", "mdl"),
        P("mdl"),
        P("mdl"),
        P("mdl", "req"),
        P(),
        P(),
        P(),
        P(),
        P("req", None),
        P("req", None, "mdl"),
        P("req", "mdl"),
        P("req", "mdl", None),
        P(),
    )
    out_specs = P("req", "mdl")
    return jax.shard_map(shards, mesh=mesh, in_specs=in_specs, out_specs=out_specs, check_vma=False)
```

```python
import functools
import math

import jax
import jax.numpy as jnp
import numpy as np
from jax import lax
from jax.experimental import pallas as pl
from jax.experimental.pallas import tpu as pltpu
from jax.sharding import PartitionSpec as P

HEAD_SIZE = 64
PAGE_POSITIONS = 128
SHORT_MAX = 256
QUERY_PER_KEY = 8
SHORT_PAGES = 2
SLOTS = 8

NX, NZ, NY, NC = 4, 8, 4, 2

norm_epsilon = 1e-05
rope_theta = 150000.0
swiglu_limit = 7.0
swiglu_alpha = 1.702

BF = jnp.bfloat16
F32 = jnp.float32
VMEM_LIMIT = 58 * 2**20
LOWEST = -1e30
MESH = pl.DeviceIdType.MESH


def place():
    r = lax.axis_index("req")
    m = lax.axis_index("mdl")
    return r, m, r // NZ, r % NZ, m // NC, m % NC


def device(r, m):
    return {"req": r, "mdl": m}


def dot(a, b):
    return jnp.dot(a, b, preferred_element_type=F32)


def dot_nt(a, b):
    return lax.dot_general(a, b, (((1,), (1,)), ((), ())), preferred_element_type=F32)


def split3(value):
    high = value.astype(BF)
    rest = value - high.astype(F32)
    middle = rest.astype(BF)
    low = (rest - middle.astype(F32)).astype(BF)
    return high, middle, low


class Ring:
    def __init__(self, size, me, ref_of, send, recv, target):
        self.size, self.me, self.ref_of = size, me, ref_of
        self.send, self.recv, self.target = send, recv, target
        self.half = size // 2
        self.plan = [
            (way, dist, part)
            for dist in range(1, self.half + 1)
            for part in range(2)
            for way in range(2)
            if self.exists(way, dist, part)
        ]

    def exists(self, way, dist, part):
        return dist < self.half or (dist == self.half and part == way)

    def index(self, way, dist, part):
        return (way * self.half + dist - 1) * 2 + part

    def origin(self, way, dist):
        return (self.me + (dist if way else self.size - dist)) % self.size

    def copy(self, way, dist, part):
        ref = self.ref_of(self.origin(way, dist - 1), part)
        i = self.index(way, dist, part)
        to = (self.me + (self.size - 1 if way else 1)) % self.size
        return pltpu.make_async_remote_copy(
            src_ref=ref,
            dst_ref=ref,
            send_sem=self.send.at[i],
            recv_sem=self.recv.at[i],
            device_id=self.target(to),
            device_id_type=MESH,
        )

    def arrive(self, way, dist, part):
        ref = self.ref_of(self.origin(way, dist), part)
        i = self.index(way, dist, part)
        pltpu.make_async_remote_copy(
            src_ref=ref,
            dst_ref=ref,
            send_sem=self.send.at[i],
            recv_sem=self.recv.at[i],
            device_id=self.target(self.me),
            device_id_type=MESH,
        ).wait_recv()

    def begin(self, part):
        for way in range(2):
            if self.exists(way, 1, part):
                self.copy(way, 1, part).start()

    def step(self, way, dist, part):
        self.arrive(way, dist, part)
        if self.exists(way, dist + 1, part):
            self.copy(way, dist + 1, part).start()

    def finish(self):
        for way, dist, part in self.plan:
            self.copy(way, dist, part).wait_send()


def remote(src, dst, send, recv, r, m):
    return pltpu.make_async_remote_copy(
        src_ref=src,
        dst_ref=dst,
        send_sem=send,
        recv_sem=recv,
        device_id=device(r, m),
        device_id_type=MESH,
    )


def ring_sems(size):
    return [pltpu.SemaphoreType.DMA((2 * size,)), pltpu.SemaphoreType.DMA((2 * size,))]


def lane_cut(width):
    tiles = width // 128
    return 128 * ((tiles + 1) // 2) if tiles > 1 else 0


def project_kernel(
    hidden, gain, wqkv, wo, bias,
    proj, wo_out,
    gathered, wo_all, parcels, rows, blocks, total, sums, sums_in,
    ring_send, ring_recv, wo_send, wo_recv, x_send, x_recv, s_send, s_recv, local,
):
    r, m, x, z, y, c = place()
    tokens, width = hidden.shape
    group = width // NX
    block = group // NZ

    load_q = pltpu.make_async_copy(wqkv, gathered.at[z], local.at[0])
    load_o = pltpu.make_async_copy(wo, wo_all.at[z], local.at[1])
    load_q.start()
    load_o.start()

    barrier = pltpu.get_barrier_semaphore()
    for step in (1, NZ - 1):
        pl.semaphore_signal(barrier, inc=1, device_id=device(x * NZ + (z + step) % NZ, m), device_id_type=MESH)
    for step in range(1, NX):
        pl.semaphore_signal(barrier, inc=1, device_id=device((x + step) % NX * NZ + z, m), device_id_type=MESH)
    load_q.wait()
    pl.semaphore_wait(barrier, NX + 1)

    cut_q, cut_o = lane_cut(wqkv.shape[1]), lane_cut(wo.shape[1])

    def part_of(buffer, cut):
        full = buffer.shape[-1]

        def ref_of(origin, part):
            return buffer.at[origin, :, pl.ds(0, cut) if part == 0 else pl.ds(cut, full - cut)]

        return ref_of

    def at_z(to):
        return device(x * NZ + to, m)

    ring = Ring(NZ, z, part_of(gathered, cut_q), ring_send, ring_recv, at_z)
    ring_o = Ring(NZ, z, part_of(wo_all, cut_o), wo_send, wo_recv, at_z)
    for part in range(2):
        ring.begin(part)

    value = hidden[...].astype(F32)
    scale = lax.rsqrt(jnp.mean(value * value, axis=-1, keepdims=True) + norm_epsilon)
    normed = (value * scale * gain[...][None, :]).astype(BF)
    for k in range(NX):
        parcels[k] = normed[:, group * k : group * k + group]

    def x_copy(src, dst, send, recv, step):
        to = (x + step) % NX
        return remote(src.at[to], dst.at[x], send.at[step], recv.at[step], to * NZ + z, m)

    def x_arrive(dst, send, recv, step):
        origin = (x + NX - step) % NX
        remote(dst.at[origin], dst.at[origin], send.at[step], recv.at[step], r, m).wait_recv()

    for step in range(1, NX):
        x_copy(parcels, rows, x_send, x_recv, step).start()
    rows[x] = parcels[x]

    for step in range(1, NX):
        x_arrive(rows, x_send, x_recv, step)
    for k in range(NZ):
        for j in range(NX):
            blocks[k, j * tokens : (j + 1) * tokens] = rows[j, :, block * k : block * k + block]

    def add(origin, first):
        product = dot(blocks[origin], gathered[origin])
        for j in range(NX):
            piece = product[j * tokens : (j + 1) * tokens]
            total[j] = piece if first else total[j] + piece

    add(z, True)
    for dist in range(1, ring.half + 1):
        for way, d, part in ring.plan:
            if d == dist:
                ring.step(way, d, part)
        if dist == ring.half - 1 or ring.half == 1:
            load_o.wait()
            for part in range(2):
                ring_o.begin(part)
        add(ring.origin(0, dist), False)
        if dist < ring.half:
            add(ring.origin(1, dist), False)

    for j in range(NX):
        sums[j] = total[j].astype(BF)
    for step in range(1, NX):
        x_copy(sums, sums_in, s_send, s_recv, step).start()
    for way, dist, part in ring_o.plan:
        ring_o.step(way, dist, part)
    result = total[x] + bias[...][None, :]
    for step in range(1, NX):
        x_arrive(sums_in, s_send, s_recv, step)
        result = result + sums_in[(x + NX - step) % NX].astype(F32)
    proj[...] = result
    for k in range(NZ):
        wo_out[k] = wo_all[k]

    ring.finish()
    ring_o.finish()
    for step in range(1, NX):
        x_copy(parcels, rows, x_send, x_recv, step).wait_send()
        x_copy(sums, sums_in, s_send, s_recv, step).wait_send()


def project(hidden, gain, wqkv, wo, bias):
    tokens, width = hidden.shape
    group = width // NX
    block, cols = wqkv.shape
    out_rows = wo.shape[1]
    vmem = pl.BlockSpec(memory_space=pltpu.VMEM)
    hbm = pl.BlockSpec(memory_space=pl.ANY)
    return pl.pallas_call(
        project_kernel,
        name="project",
        out_shape=(
            jax.ShapeDtypeStruct((tokens, cols), F32),
            jax.ShapeDtypeStruct((NZ, block, out_rows), BF),
        ),
        in_specs=[vmem, vmem, hbm, hbm, vmem],
        out_specs=(vmem, vmem),
        scratch_shapes=[
            pltpu.VMEM((NZ, block, cols), BF),
            pltpu.VMEM((NZ, block, out_rows), BF),
            pltpu.VMEM((NX, tokens, group), BF),
            pltpu.VMEM((NX, tokens, group), BF),
            pltpu.VMEM((NZ, NX * tokens, block), BF),
            pltpu.VMEM((NX, tokens, cols), F32),
            pltpu.VMEM((NX, tokens, cols), BF),
            pltpu.VMEM((NX, tokens, cols), BF),
            *ring_sems(NZ),
            *ring_sems(NZ),
            *[pltpu.SemaphoreType.DMA((NX,))] * 4,
            pltpu.SemaphoreType.DMA((2,)),
        ],
        compiler_params=pltpu.CompilerParams(
            collective_id=1, has_side_effects=True, vmem_limit_bytes=VMEM_LIMIT
        ),
    )(hidden, gain, wqkv, wo, bias)


def find_long(lengths, count, most_long, rank, at_long):
    def see(i, carry):
        seen, places = carry
        rank[i] = jnp.minimum(seen, most_long - 1)
        seen = seen + (lengths[i] > SHORT_MAX).astype(jnp.int32)
        return seen, tuple(p + (seen <= j).astype(jnp.int32) for j, p in enumerate(places))

    zero = jnp.int32(0)
    _, places = lax.fori_loop(0, count, see, (zero, (zero,) * most_long))
    for j in range(most_long):
        at_long[j] = jnp.minimum(places[j], count - 1)


def attend_kernel(
    lengths, table, proj, cosines, sines, sinks, cache,
    out,
    pool, rank, at_long, scores, far_scores, queries, owns, tops, bottoms, mixed,
    far_top, far_bottom, far_mixed, load,
):
    r = lax.axis_index("req")
    load_pool = pltpu.make_async_copy(cache, pool, load.at[0])
    load_pool.start()
    count = proj.shape[0]
    heads = QUERY_PER_KEY
    most_long = far_scores.shape[0]
    find_long(lengths, count, most_long, rank, at_long)
    pages = table.shape[0]
    channels = pool.shape[2]
    score_scale = 1.0 / math.sqrt(HEAD_SIZE)
    base = r * pool.shape[0]

    value = proj[...]
    lanes = lax.broadcasted_iota(jnp.int32, value.shape, 1)
    width = value.shape[1]
    first = (lanes % HEAD_SIZE) < HEAD_SIZE // 2
    partner = jnp.where(
        first,
        pltpu.roll(value, width - HEAD_SIZE // 2, axis=1),
        pltpu.roll(value, HEAD_SIZE // 2, axis=1),
    )
    repeat = width // cosines.shape[1]
    turned = value * jnp.concatenate([cosines[...]] * repeat, axis=1) + partner * jnp.concatenate(
        [sines[...]] * repeat, axis=1
    )
    key_at = heads * HEAD_SIZE
    rounded = jnp.where(lanes < key_at + HEAD_SIZE, turned, value).astype(BF).astype(F32)
    new_key = rounded[:, key_at : key_at + HEAD_SIZE]
    new_value = rounded[:, key_at + HEAD_SIZE :]
    queries[...] = jnp.zeros_like(queries)
    for h in range(heads):
        head = rounded[:, h * HEAD_SIZE : (h + 1) * HEAD_SIZE]
        queries[:, h, 0:HEAD_SIZE] = head
        own = jnp.sum(head * new_key, axis=1, keepdims=True) * score_scale
        owns[:, h, :] = jnp.broadcast_to(own, (count, channels))
    load_pool.wait()

    def entries(i, start, stop):
        return jnp.concatenate(
            [pool[jnp.clip(table[p, i] - base, 0, pool.shape[0] - 1)] for p in range(start, stop)], axis=0
        )

    def masked(raw, i, start):
        positions = lax.broadcasted_iota(jnp.int32, raw.shape, 1) + start
        return jnp.where(positions < lengths[i], raw * score_scale, LOWEST)

    at_once = 8 if count % 8 == 0 else 1

    def score(g, carry):
        for u in range(at_once):
            i = g * at_once + u
            scores[i] = masked(dot_nt(queries[i].astype(BF), entries(i, 0, SHORT_PAGES)), i, 0)
        return carry

    lax.fori_loop(0, count // at_once, score, 0)

    def far_score(j, carry):
        i = at_long[j]
        far_scores[j] = masked(dot_nt(queries[i].astype(BF), entries(i, SHORT_PAGES, pages)), i, SHORT_MAX)
        return carry

    lax.fori_loop(0, most_long, far_score, 0)

    def weigh(held, tops, bottoms):
        raw = held[...]
        top = jnp.max(raw, axis=2, keepdims=True)
        weight = jnp.exp(raw - top)
        held[...] = weight
        tops[...] = jnp.broadcast_to(top, tops.shape)
        bottoms[...] = jnp.broadcast_to(jnp.sum(weight, axis=2, keepdims=True), bottoms.shape)

    weigh(scores, tops, bottoms)
    weigh(far_scores, far_top, far_bottom)

    def mix(g, carry):
        for u in range(at_once):
            i = g * at_once + u
            mixed[i] = dot(scores[i].astype(BF), entries(i, 0, SHORT_PAGES))
        return carry

    lax.fori_loop(0, count // at_once, mix, 0)

    def far_mix(j, carry):
        far_mixed[j] = dot(far_scores[j].astype(BF), entries(at_long[j], SHORT_PAGES, pages))
        return carry

    lax.fori_loop(0, most_long, far_mix, 0)

    sink_rows = lax.broadcasted_iota(jnp.int32, (heads, channels), 0)
    sink = jnp.zeros((heads, channels), F32)
    for h in range(heads):
        sink = jnp.where(sink_rows == h, sinks[h], sink)

    def join(g, carry):
        for u in range(at_once):
            i = g * at_once + u
            k = rank[i]
            is_long = jnp.full((heads, channels), lengths[i], jnp.int32) > SHORT_MAX
            far = jnp.where(is_long, far_top[k], LOWEST)
            own = owns[i]
            near = tops[i]
            top = jnp.maximum(jnp.maximum(near, far), jnp.maximum(own, sink))
            near_scale = jnp.exp(near - top)
            far_scale = jnp.exp(far - top)
            own_weight = jnp.exp(own - top)
            bottom = bottoms[i] * near_scale + own_weight + jnp.exp(sink - top)
            bottom = bottom + jnp.where(is_long, far_bottom[k] * far_scale, 0.0)
            both = mixed[i] * near_scale + jnp.where(is_long, far_mixed[k] * far_scale, 0.0)
            mixed[i] = both / bottom
            owns[i] = own_weight / bottom
        return carry

    lax.fori_loop(0, count // at_once, join, 0)
    for h in range(heads):
        head = mixed[:, h, HEAD_SIZE:] + owns[:, h, 0:1] * new_value
        out[:, h * HEAD_SIZE : (h + 1) * HEAD_SIZE] = head.astype(BF)


def attend(lengths, table, proj, cosines, sines, sinks, cache):
    tokens = proj.shape[0]
    channels = cache.shape[2]
    pages = table.shape[0]
    most_long = tokens // 4
    vmem = pl.BlockSpec(memory_space=pltpu.VMEM)
    smem = pl.BlockSpec(memory_space=pltpu.SMEM)
    per_head = pltpu.VMEM((tokens, QUERY_PER_KEY, channels), F32)
    per_long = pltpu.VMEM((most_long, QUERY_PER_KEY, channels), F32)
    return pl.pallas_call(
        attend_kernel,
        name="attend",
        out_shape=jax.ShapeDtypeStruct((tokens, QUERY_PER_KEY * HEAD_SIZE), BF),
        in_specs=[smem, smem, vmem, vmem, vmem, smem, pl.BlockSpec(memory_space=pl.ANY)],
        out_specs=vmem,
        scratch_shapes=[
            pltpu.VMEM(cache.shape, BF),
            pltpu.SMEM((tokens,), jnp.int32),
            pltpu.SMEM((most_long,), jnp.int32),
            pltpu.VMEM((tokens, QUERY_PER_KEY, SHORT_PAGES * PAGE_POSITIONS), F32),
            pltpu.VMEM((most_long, QUERY_PER_KEY, (pages - SHORT_PAGES) * PAGE_POSITIONS), F32),
            *[per_head] * 5,
            *[per_long] * 3,
            pltpu.SemaphoreType.DMA((1,)),
        ],
        compiler_params=pltpu.CompilerParams(vmem_limit_bytes=VMEM_LIMIT),
    )(lengths, table, proj, cosines, sines, sinks, cache)


def expert_kernel(
    att, wo_all, hidden, obias, egain, router, router_bias, routes_t, w1_hbm, b1, w2_hbm, rbias,
    out,
    w1, w2, heads, halves, summed, mine, outgoing, gathered, full, pre, near_out, near_in, far_out, far_in,
    kept, back_out, back_in, logits_out, logits_in, share_f32, gains,
    x_send, x_recv, s_send, s_recv, d_send, d_recv, ring_send, ring_recv, p_send, p_recv,
    n_send, n_recv, f_send, f_recv, b_send, b_recv, l_send, l_recv, local,
):
    r, m, x, z, y, c = place()
    tokens, width = hidden.shape
    count_req, count_mdl = NX * NZ, NY * NC
    share = width // count_mdl
    block = width // count_req
    padded = outgoing.shape[2]
    rows = count_req * SLOTS
    per_group = NZ * block // share

    load1 = pltpu.make_async_copy(w1_hbm, w1, local.at[0])
    load2 = pltpu.make_async_copy(w2_hbm, w2, local.at[1])
    load1.start()
    load2.start()

    barrier = pltpu.get_barrier_semaphore()

    def greet(to_r, to_m):
        pl.semaphore_signal(barrier, inc=1, device_id=device(to_r, to_m), device_id_type=MESH)

    def greet_req(step, carry):
        greet((r + step) % count_req, m)
        return carry

    lax.fori_loop(1, count_req, greet_req, 0)
    for step in range(1, count_mdl):
        greet(r, (m + step) % count_mdl)
    diagonal = x == y
    for step in range(NX):
        for j in range(per_group):
            not_me = jnp.logical_or(step > 0, per_group * x + j != m)

            @pl.when(not_me)
            def _():
                greet((x + step) % NX * NZ + z, per_group * x + j)

    for j in range(count_mdl):

        @pl.when(jnp.logical_not(jnp.logical_and(diagonal, m == j)))
        def _():
            greet(y * NZ + z, j)

    pl.semaphore_wait(
        barrier,
        (count_req - 1) + (count_mdl - 1) + NX * per_group + count_mdl - 2 * diagonal.astype(jnp.int32),
    )

    for step in range(1, NX):
        to = (x + step) % NX
        remote(att, heads.at[x], x_send.at[step], x_recv.at[step], to * NZ + z, m).start()
    heads[x] = att[...]

    obias_row, egain_row = obias[...][None, :], egain[...][None, :]
    for k in range(count_mdl):

        @pl.when(m == k)
        def _():
            at = slice(share * k, share * k + share)
            share_f32[...] = hidden[:, at].astype(F32) + obias_row[:, at]
            gains[0:1, :] = egain_row[:, at]
            gains[8 : 8 + count_req, :] = rbias[:, at]
            gains[8 + count_req : 8 + 2 * count_req, :] = router[:, at].astype(F32)

    names = lax.broadcasted_iota(jnp.int32, (count_req, tokens), 0)
    hot_t = jnp.zeros((count_req, tokens), F32)
    for k in range(routes_t.shape[0]):
        hot_t = hot_t + (routes_t[k : k + 1, :] == names).astype(F32)
    same = lax.broadcasted_iota(jnp.int32, (tokens, tokens), 0) == lax.broadcasted_iota(
        jnp.int32, (tokens, tokens), 1
    )
    hot = dot_nt(same.astype(BF), hot_t.astype(BF))
    before = lax.broadcasted_iota(jnp.int32, (tokens, tokens), 0) < lax.broadcasted_iota(
        jnp.int32, (tokens, tokens), 1
    )
    rank_t = dot(hot_t.astype(BF), before.astype(BF))
    after = lax.broadcasted_iota(jnp.int32, (tokens, tokens), 0) > lax.broadcasted_iota(
        jnp.int32, (tokens, tokens), 1
    )
    rank = dot(after.astype(BF), hot.astype(BF))
    spread = (
        lax.broadcasted_iota(jnp.int32, (rows, count_req), 0) // SLOTS
        == lax.broadcasted_iota(jnp.int32, (rows, count_req), 1)
    ).astype(BF)
    spread_t = (
        lax.broadcasted_iota(jnp.int32, (count_req, rows), 1) // SLOTS
        == lax.broadcasted_iota(jnp.int32, (count_req, rows), 0)
    ).astype(BF)
    slot = (lax.broadcasted_iota(jnp.int32, (rows, tokens), 0) % SLOTS).astype(F32)
    place_rows = jnp.where(
        jnp.logical_and(dot(spread, hot_t.astype(BF)) > 0.5, dot(spread, rank_t.astype(BF)) == slot), 1.0, 0.0
    ).astype(BF)
    slot_t = (lax.broadcasted_iota(jnp.int32, (tokens, rows), 1) % SLOTS).astype(F32)
    take_rows = jnp.where(
        jnp.logical_and(dot(hot.astype(BF), spread_t) > 0.5, dot(rank.astype(BF), spread_t) == slot_t), 1.0, 0.0
    )

    for step in range(1, NX):
        origin = (x + NX - step) % NX
        remote(heads.at[origin], heads.at[origin], x_send.at[step], x_recv.at[step], r, m).wait_recv()

    stacked = jnp.concatenate([heads[j] for j in range(NX)], axis=0)
    per_share = share // block
    for k in range(NZ):
        product = dot_nt(stacked, wo_all[k]).astype(BF)
        for j in range(NX):
            halves[k // per_share, j, :, block * (k % per_share) : block * (k % per_share) + block] = product[
                j * tokens : (j + 1) * tokens
            ]

    def sum_copy(step, j):
        to = (x + step) % NX
        i = step * per_group + j
        return remote(
            halves.at[j, to], summed.at[m], s_send.at[i], s_recv.at[m], to * NZ + z, per_group * x + j
        )

    for step in range(NX):
        for j in range(per_group):

            @pl.when(jnp.logical_or(step > 0, per_group * x + j != m))
            def _():
                sum_copy(step, j).start()

    @pl.when(diagonal)
    def _():
        summed[m] = halves[m % per_group, x]

    residual = share_f32[...]
    for j in range(count_mdl):

        @pl.when(jnp.logical_not(jnp.logical_and(diagonal, m == j)))
        def _():
            remote(summed.at[j], summed.at[j], s_send.at[0], s_recv.at[j], r, m).wait_recv()

    total = summed[0].astype(F32)
    for j in range(1, count_mdl):
        total = total + summed[j].astype(F32)
    residual = (residual + total).astype(BF).astype(F32)
    share_f32[...] = residual
    squares = jnp.sum(residual * residual, axis=1, keepdims=True)
    scaled = (residual * gains[0:1, :]).astype(BF)
    mine[...] = jnp.zeros_like(mine)
    mine[:, 0:share] = scaled
    for k, piece in enumerate(split3(squares)):
        mine[:, share + k : share + k + 1] = piece

    outgoing[...] = dot(place_rows, mine[...]).astype(BF).reshape(outgoing.shape)

    def send_row(step, carry):
        to = (r + step) % count_req
        remote(outgoing.at[to], gathered.at[m, r], d_send.at[step], d_recv.at[r], to, m).start()
        return carry

    lax.fori_loop(1, count_req, send_row, 0)
    gathered[m, r] = outgoing[r]

    routing = gains[8 + count_req : 8 + 2 * count_req, :].astype(BF)
    logits_out[...] = jnp.zeros_like(logits_out)
    logits_out[:, 0:count_req] = dot_nt(scaled, routing)
    logits_out[:, count_req : count_req + 1] = squares
    for step in range(1, count_mdl):
        to = (m + step) % count_mdl
        remote(logits_out, logits_in.at[m], l_send.at[step], l_recv.at[step], r, to).start()
    logits_in[m] = logits_out[...]

    part_rows = count_req // 2

    def part_ref(origin, part):
        return gathered.at[origin * NC + c, pl.ds(part * part_rows, part_rows)]

    def at_y(to):
        return device(r, to * NC + c)

    ring = Ring(NY, y, part_ref, ring_send, ring_recv, at_y)

    def pair_index(way, dist):
        return way * ring.half + dist

    def pair_copy(way, dist, part):
        origin = ring.origin(way, dist)
        ref = part_ref(origin, part)
        i = pair_index(way, dist) * 2 + part
        return remote(ref, ref, p_send.at[i], p_recv.at[i], r, y * NC + 1 - c)

    def pair_arrive(way, dist, part):
        ref = gathered.at[ring.origin(way, dist) * NC + 1 - c, pl.ds(part * part_rows, part_rows)]
        i = pair_index(way, dist) * 2 + part
        remote(ref, ref, p_send.at[i], p_recv.at[i], r, m).wait_recv()

    for part in range(2):

        def take(origin, carry):
            @pl.when(origin != r)
            def _():
                remote(gathered.at[m, origin], gathered.at[m, origin], d_send.at[0], d_recv.at[origin], r, m).wait_recv()

            return carry

        lax.fori_loop(part * part_rows, (part + 1) * part_rows, take, 0)
        ring.begin(part)
        pair_copy(0, 0, part).start()

    for way, dist, part in ring.plan:
        ring.step(way, dist, part)
        pair_copy(way, dist, part).start()
    pair_plan = [(0, 0, 0), (0, 0, 1)] + ring.plan
    for way, dist, part in pair_plan:
        pair_arrive(way, dist, part)

    load1.wait()
    load2.wait()
    square_sum = jnp.zeros((rows, 1), F32)
    for k in range(count_mdl):
        piece = gathered[k].reshape(rows, padded)
        full[:, share * k : share * k + share] = piece[:, 0:share]
        for j in range(3):
            square_sum = square_sum + piece[:, share + j : share + j + 1].astype(F32)
    root = lax.rsqrt(square_sum * (1.0 / width) + norm_epsilon)
    columns = w1.shape[0]
    pre[...] = jnp.zeros_like(pre)
    pre[:, 0:columns] = dot_nt(full[...], w1[...]) * root + b1[...]
    raw = pre[...]
    up = jnp.clip(pltpu.roll(raw, raw.shape[1] - 1, axis=1), -swiglu_limit, swiglu_limit)
    gate = jnp.minimum(raw, swiglu_limit)
    act = (gate * jax.nn.sigmoid(swiglu_alpha * gate) * (up + 1.0)).astype(BF)
    hidden_units = columns // 2
    pick = (
        lax.broadcasted_iota(jnp.int32, (raw.shape[1], hidden_units), 0)
        == 2 * lax.broadcasted_iota(jnp.int32, (raw.shape[1], hidden_units), 1)
    ).astype(BF)
    act = dot(act, pick).astype(BF)

    def produce(k):
        return dot(act, w2[:, share * k : share * k + share])

    def near_copy(k):
        return remote(near_out.at[k], near_in.at[k], n_send.at[k], n_recv.at[k], r, y * NC + 1 - c)

    for core in range(NC):

        @pl.when(c == core)
        def _():
            for k in range(NY):
                near_out[k] = produce(k * NC + 1 - core).astype(BF)
                near_copy(k).start()
            for k in range(NY):
                kept[k] = produce(k * NC + core)

    def far_copy(step):
        to = (y + step) % NY
        return remote(far_out.at[to], far_in.at[y], f_send.at[step], f_recv.at[step], r, to * NC + c)

    for step in range(1, NY):
        to = (y + step) % NY
        remote(near_in.at[to], near_in.at[to], n_send.at[to], n_recv.at[to], r, m).wait_recv()
        far_out[to] = (kept[to] + near_in[to].astype(F32)).astype(BF)
        far_copy(step).start()
    remote(near_in.at[y], near_in.at[y], n_send.at[y], n_recv.at[y], r, m).wait_recv()
    answer = kept[y] + near_in[y].astype(F32)
    for step in range(1, NY):
        origin = (y + NY - step) % NY
        remote(far_in.at[origin], far_in.at[origin], f_send.at[step], f_recv.at[step], r, m).wait_recv()
        answer = answer + far_in[origin].astype(F32)
    back_out[...] = answer.astype(BF).reshape(back_out.shape)

    def send_back(step, carry):
        to = (r + step) % count_req
        remote(back_out.at[to], back_in.at[r], b_send.at[step], b_recv.at[step], to, m).start()
        return carry

    lax.fori_loop(1, count_req, send_back, 0)
    back_in[r] = back_out[r]

    for step in range(1, count_mdl):
        origin = (m + count_mdl - step) % count_mdl
        remote(logits_in.at[origin], logits_in.at[origin], l_send.at[step], l_recv.at[step], r, m).wait_recv()
    both = logits_in[0]
    for k in range(1, count_mdl):
        both = both + logits_in[k]
    row_root = lax.rsqrt(both[:, count_req : count_req + 1] * (1.0 / width) + norm_epsilon)
    logits = both[:, 0:count_req] * row_root + router_bias[...]
    logits = jnp.where(hot > 0.5, logits, -jnp.inf)
    weight = jnp.exp(logits - jnp.max(logits, axis=1, keepdims=True))
    gates = weight / jnp.sum(weight, axis=1, keepdims=True)
    result = share_f32[...]
    biases = split3(gains[8 : 8 + count_req, :])
    gate_parts = split3(gates)
    for i in range(3):
        for j in range(3 - i):
            result = result + dot(gate_parts[i], biases[j])
    takers = [(take_rows * dot(piece, spread_t)).astype(BF) for piece in gate_parts]

    def take_back(step, carry):
        origin = (r + count_req - step) % count_req
        remote(back_in.at[origin], back_in.at[origin], b_send.at[step], b_recv.at[step], r, m).wait_recv()
        return carry

    lax.fori_loop(1, count_req, take_back, 0)
    returned = back_in[...].reshape(rows, share)
    for taker in takers:
        result = result + dot(taker, returned)
    out[...] = result.astype(BF)

    for step in range(1, NX):
        to = (x + step) % NX
        remote(att, heads.at[x], x_send.at[step], x_recv.at[step], to * NZ + z, m).wait_send()
    for step in range(NX):
        for j in range(per_group):

            @pl.when(jnp.logical_or(step > 0, per_group * x + j != m))
            def _():
                sum_copy(step, j).wait_send()

    def sent(step, carry):
        to = (r + step) % count_req
        remote(outgoing.at[to], gathered.at[m, r], d_send.at[step], d_recv.at[r], to, m).wait_send()
        remote(back_out.at[to], back_in.at[r], b_send.at[step], b_recv.at[step], to, m).wait_send()
        return carry

    lax.fori_loop(1, count_req, sent, 0)
    ring.finish()
    for way, dist, part in pair_plan:
        pair_copy(way, dist, part).wait_send()
    for k in range(NY):
        near_copy(k).wait_send()
    for step in range(1, NY):
        far_copy(step).wait_send()
    for step in range(1, count_mdl):
        to = (m + step) % count_mdl
        remote(logits_out, logits_in.at[m], l_send.at[step], l_recv.at[step], r, to).wait_send()


def experts(att, wo_all, hidden, obias, egain, router, router_bias, routes_t, w1, b1, w2, rbias):
    tokens, width = hidden.shape
    count_req, count_mdl = NX * NZ, NY * NC
    share = width // count_mdl
    padded = -(-(share + 3) // 128) * 128
    rows = count_req * SLOTS
    columns = w1.shape[0]
    wide = -(-(columns + 1) // 128) * 128
    per_group = count_mdl // NX
    vmem = pl.BlockSpec(memory_space=pltpu.VMEM)
    hbm = pl.BlockSpec(memory_space=pl.ANY)
    dma = pltpu.SemaphoreType.DMA
    return pl.pallas_call(
        expert_kernel,
        name="experts",
        out_shape=jax.ShapeDtypeStruct((tokens, share), BF),
        in_specs=[vmem] * 8 + [hbm, vmem, hbm, vmem],
        out_specs=vmem,
        scratch_shapes=[
            pltpu.VMEM(w1.shape, BF),
            pltpu.VMEM(w2.shape, BF),
            pltpu.VMEM((NX,) + att.shape, BF),
            pltpu.VMEM((per_group, NX, tokens, share), BF),
            pltpu.VMEM((count_mdl, tokens, share), BF),
            pltpu.VMEM((tokens, padded), BF),
            pltpu.VMEM((count_req, SLOTS, padded), BF),
            pltpu.VMEM((count_mdl, count_req, SLOTS, padded), BF),
            pltpu.VMEM((rows, width), BF),
            pltpu.VMEM((rows, wide), F32),
            pltpu.VMEM((NY, rows, share), BF),
            pltpu.VMEM((NY, rows, share), BF),
            pltpu.VMEM((NY, rows, share), BF),
            pltpu.VMEM((NY, rows, share), BF),
            pltpu.VMEM((NY, rows, share), F32),
            pltpu.VMEM((count_req, SLOTS, share), BF),
            pltpu.VMEM((count_req, SLOTS, share), BF),
            pltpu.VMEM((tokens, 128), F32),
            pltpu.VMEM((count_mdl, tokens, 128), F32),
            pltpu.VMEM((tokens, share), F32),
            pltpu.VMEM((8 + 2 * count_req, share), F32),
            dma((NX,)), dma((NX,)),
            dma((NX * per_group,)), dma((count_mdl,)),
            dma((count_req,)), dma((count_req,)),
            *ring_sems(NY),
            dma((2 * (NY + 2),)), dma((2 * (NY + 2),)),
            dma((NY,)), dma((NY,)),
            dma((NY,)), dma((NY,)),
            dma((count_req,)), dma((count_req,)),
            dma((count_mdl,)), dma((count_mdl,)),
            dma((2,)),
        ],
        compiler_params=pltpu.CompilerParams(
            collective_id=2, has_side_effects=True, vmem_limit_bytes=VMEM_LIMIT
        ),
    )(att, wo_all, hidden, obias, egain, router, router_bias, routes_t, w1, b1, w2, rbias)


def rotation_tables(lengths, repeat):
    half = HEAD_SIZE // 2
    frequency = np.power(rope_theta, -np.arange(half) * (2.0 / HEAD_SIZE))
    frequency = np.tile(frequency, 2 * repeat).astype(np.float32)
    sign = np.tile(np.repeat(np.float32([-1.0, 1.0]), half), repeat)
    angles = lengths.astype(F32)[:, None] * frequency[None, :]
    return jnp.cos(angles), jnp.sin(angles) * sign[None, :]


def shards(
    hidden_state,
    cached_length_list,
    page_table,
    paged_cache_store,
    attention_gain,
    qkv_weight,
    qkv_bias,
    sink_logit_values,
    output_weight,
    output_bias,
    expert_gain,
    router_weight,
    router_bias,
    expert_routes,
    expand_weight,
    expand_bias,
    reduce_weight,
    reduce_bias,
):
    projected, wo_all = project(
        hidden_state, attention_gain, qkv_weight, output_weight.T, qkv_bias
    )
    cosines, sines = rotation_tables(cached_length_list, 2)
    attended = attend(
        cached_length_list, page_table.T, projected, cosines, sines, sink_logit_values, paged_cache_store
    )
    return experts(
        attended,
        wo_all,
        hidden_state,
        output_bias,
        expert_gain,
        router_weight.T,
        router_bias[None],
        expert_routes.T,
        expand_weight[0].T,
        expand_bias,
        reduce_weight[0],
        reduce_bias,
    )


def solution(mesh):
    in_specs = (
        P("req", None),
        P("req"),
        P("req", None),
        P("req", None, "mdl"),
        P(),
        P("req", "mdl"),
        P("mdl"),
        P("mdl"),
        P("mdl", "req"),
        P(),
        P(),
        P(),
        P(),
        P("req", None),
        P("req", None, "mdl"),
        P("req", "mdl"),
        P("req", "mdl", None),
        P(),
    )
    out_specs = P("req", "mdl")
    return jax.shard_map(shards, mesh=mesh, in_specs=in_specs, out_specs=out_specs, check_vma=False)
```

```python
import functools
import math

import jax
import jax.numpy as jnp
import numpy as np
from jax import lax
from jax.experimental import pallas as pl
from jax.experimental.pallas import tpu as pltpu
from jax.sharding import PartitionSpec as P

HEAD_SIZE = 64
PAGE_POSITIONS = 128
SHORT_MAX = 256
QUERY_PER_KEY = 8
SHORT_PAGES = 2
SLOTS = 8

NX, NZ, NY, NC = 4, 8, 4, 2

norm_epsilon = 1e-05
rope_theta = 150000.0
swiglu_limit = 7.0
swiglu_alpha = 1.702

BF = jnp.bfloat16
F32 = jnp.float32
VMEM_LIMIT = 58 * 2**20
LOWEST = -1e30
MESH = pl.DeviceIdType.MESH


def place():
    r = lax.axis_index("req")
    m = lax.axis_index("mdl")
    return r, m, r // NZ, r % NZ, m // NC, m % NC


def device(r, m):
    return {"req": r, "mdl": m}


def dot(a, b):
    return jnp.dot(a, b, preferred_element_type=F32)


def dot_nt(a, b):
    return lax.dot_general(a, b, (((1,), (1,)), ((), ())), preferred_element_type=F32)


def split3(value):
    high = value.astype(BF)
    rest = value - high.astype(F32)
    middle = rest.astype(BF)
    low = (rest - middle.astype(F32)).astype(BF)
    return high, middle, low


class Ring:
    def __init__(self, size, me, ref_of, send, recv, target):
        self.size, self.me, self.ref_of = size, me, ref_of
        self.send, self.recv, self.target = send, recv, target
        self.half = size // 2
        self.plan = [
            (way, dist, part)
            for dist in range(1, self.half + 1)
            for part in range(2)
            for way in range(2)
            if self.exists(way, dist, part)
        ]

    def exists(self, way, dist, part):
        return dist < self.half or (dist == self.half and part == way)

    def index(self, way, dist, part):
        return (way * self.half + dist - 1) * 2 + part

    def origin(self, way, dist):
        return (self.me + (dist if way else self.size - dist)) % self.size

    def copy(self, way, dist, part):
        ref = self.ref_of(self.origin(way, dist - 1), part)
        i = self.index(way, dist, part)
        to = (self.me + (self.size - 1 if way else 1)) % self.size
        return pltpu.make_async_remote_copy(
            src_ref=ref,
            dst_ref=ref,
            send_sem=self.send.at[i],
            recv_sem=self.recv.at[i],
            device_id=self.target(to),
            device_id_type=MESH,
        )

    def arrive(self, way, dist, part):
        ref = self.ref_of(self.origin(way, dist), part)
        i = self.index(way, dist, part)
        pltpu.make_async_remote_copy(
            src_ref=ref,
            dst_ref=ref,
            send_sem=self.send.at[i],
            recv_sem=self.recv.at[i],
            device_id=self.target(self.me),
            device_id_type=MESH,
        ).wait_recv()

    def begin(self, part):
        for way in range(2):
            if self.exists(way, 1, part):
                self.copy(way, 1, part).start()

    def step(self, way, dist, part):
        self.arrive(way, dist, part)
        if self.exists(way, dist + 1, part):
            self.copy(way, dist + 1, part).start()

    def finish(self):
        for way, dist, part in self.plan:
            self.copy(way, dist, part).wait_send()


def remote(src, dst, send, recv, r, m):
    return pltpu.make_async_remote_copy(
        src_ref=src,
        dst_ref=dst,
        send_sem=send,
        recv_sem=recv,
        device_id=device(r, m),
        device_id_type=MESH,
    )


def ring_sems(size):
    return [pltpu.SemaphoreType.DMA((2 * size,)), pltpu.SemaphoreType.DMA((2 * size,))]


def lane_cut(width):
    tiles = width // 128
    return 128 * ((tiles + 1) // 2) if tiles > 1 else 0


def project_kernel(
    hidden, gain, wqkv, wo, bias,
    proj, wo_out,
    gathered, wo_all, parcels, rows, blocks, total, sums, sums_in,
    ring_send, ring_recv, wo_send, wo_recv, x_send, x_recv, s_send, s_recv, local,
):
    r, m, x, z, y, c = place()
    tokens, width = hidden.shape
    group = width // NX
    block = group // NZ

    load_q = pltpu.make_async_copy(wqkv, gathered.at[z], local.at[0])
    load_o = pltpu.make_async_copy(wo, wo_all.at[z], local.at[1])
    load_q.start()
    load_o.start()

    barrier = pltpu.get_barrier_semaphore()
    for step in (1, NZ - 1):
        pl.semaphore_signal(barrier, inc=1, device_id=device(x * NZ + (z + step) % NZ, m), device_id_type=MESH)
    for step in range(1, NX):
        pl.semaphore_signal(barrier, inc=1, device_id=device((x + step) % NX * NZ + z, m), device_id_type=MESH)
    load_q.wait()
    pl.semaphore_wait(barrier, NX + 1)

    cut_q, cut_o = lane_cut(wqkv.shape[1]), lane_cut(wo.shape[1])

    def part_of(buffer, cut):
        full = buffer.shape[-1]

        def ref_of(origin, part):
            return buffer.at[origin, :, pl.ds(0, cut) if part == 0 else pl.ds(cut, full - cut)]

        return ref_of

    def at_z(to):
        return device(x * NZ + to, m)

    ring = Ring(NZ, z, part_of(gathered, cut_q), ring_send, ring_recv, at_z)
    ring_o = Ring(NZ, z, part_of(wo_all, cut_o), wo_send, wo_recv, at_z)
    for part in range(2):
        ring.begin(part)

    value = hidden[...].astype(F32)
    scale = lax.rsqrt(jnp.mean(value * value, axis=-1, keepdims=True) + norm_epsilon)
    normed = (value * scale * gain[...][None, :]).astype(BF)
    for k in range(NX):
        parcels[k] = normed[:, group * k : group * k + group]

    def x_copy(src, dst, send, recv, step):
        to = (x + step) % NX
        return remote(src.at[to], dst.at[x], send.at[step], recv.at[step], to * NZ + z, m)

    def x_arrive(dst, send, recv, step):
        origin = (x + NX - step) % NX
        remote(dst.at[origin], dst.at[origin], send.at[step], recv.at[step], r, m).wait_recv()

    for step in range(1, NX):
        x_copy(parcels, rows, x_send, x_recv, step).start()
    rows[x] = parcels[x]

    for step in range(1, NX):
        x_arrive(rows, x_send, x_recv, step)
    for k in range(NZ):
        for j in range(NX):
            blocks[k, j * tokens : (j + 1) * tokens] = rows[j, :, block * k : block * k + block]

    def add(origin, first):
        product = dot(blocks[origin], gathered[origin])
        for j in range(NX):
            piece = product[j * tokens : (j + 1) * tokens]
            total[j] = piece if first else total[j] + piece

    add(z, True)
    for dist in range(1, ring.half + 1):
        for way, d, part in ring.plan:
            if d == dist:
                ring.step(way, d, part)
        if dist == ring.half - 1 or ring.half == 1:
            load_o.wait()
            for part in range(2):
                ring_o.begin(part)
        add(ring.origin(0, dist), False)
        if dist < ring.half:
            add(ring.origin(1, dist), False)

    for j in range(NX):
        sums[j] = total[j].astype(BF)
    for step in range(1, NX):
        x_copy(sums, sums_in, s_send, s_recv, step).start()
    for way, dist, part in ring_o.plan:
        ring_o.step(way, dist, part)
    result = total[x] + bias[...][None, :]
    for step in range(1, NX):
        x_arrive(sums_in, s_send, s_recv, step)
        result = result + sums_in[(x + NX - step) % NX].astype(F32)
    proj[...] = result
    for k in range(NZ):
        wo_out[k] = wo_all[k]

    ring.finish()
    ring_o.finish()
    for step in range(1, NX):
        x_copy(parcels, rows, x_send, x_recv, step).wait_send()
        x_copy(sums, sums_in, s_send, s_recv, step).wait_send()


def project(hidden, gain, wqkv, wo, bias):
    tokens, width = hidden.shape
    group = width // NX
    block, cols = wqkv.shape
    out_rows = wo.shape[1]
    vmem = pl.BlockSpec(memory_space=pltpu.VMEM)
    hbm = pl.BlockSpec(memory_space=pl.ANY)
    return pl.pallas_call(
        project_kernel,
        name="project",
        out_shape=(
            jax.ShapeDtypeStruct((tokens, cols), F32),
            jax.ShapeDtypeStruct((NZ, block, out_rows), BF),
        ),
        in_specs=[vmem, vmem, hbm, hbm, vmem],
        out_specs=(vmem, vmem),
        scratch_shapes=[
            pltpu.VMEM((NZ, block, cols), BF),
            pltpu.VMEM((NZ, block, out_rows), BF),
            pltpu.VMEM((NX, tokens, group), BF),
            pltpu.VMEM((NX, tokens, group), BF),
            pltpu.VMEM((NZ, NX * tokens, block), BF),
            pltpu.VMEM((NX, tokens, cols), F32),
            pltpu.VMEM((NX, tokens, cols), BF),
            pltpu.VMEM((NX, tokens, cols), BF),
            *ring_sems(NZ),
            *ring_sems(NZ),
            *[pltpu.SemaphoreType.DMA((NX,))] * 4,
            pltpu.SemaphoreType.DMA((2,)),
        ],
        compiler_params=pltpu.CompilerParams(
            collective_id=1, has_side_effects=True, vmem_limit_bytes=VMEM_LIMIT
        ),
    )(hidden, gain, wqkv, wo, bias)


def find_long(lengths, count, most_long, rank, at_long):
    def see(i, carry):
        seen, places = carry
        rank[i] = jnp.minimum(seen, most_long - 1)
        seen = seen + (lengths[i] > SHORT_MAX).astype(jnp.int32)
        return seen, tuple(p + (seen <= j).astype(jnp.int32) for j, p in enumerate(places))

    zero = jnp.int32(0)
    _, places = lax.fori_loop(0, count, see, (zero, (zero,) * most_long))
    for j in range(most_long):
        at_long[j] = jnp.minimum(places[j], count - 1)


def attend_kernel(
    lengths, table, proj, cosines, sines, sinks, cache,
    out,
    pool, rank, at_long, scores, far_scores, queries, owns, tops, bottoms, mixed,
    far_top, far_bottom, far_mixed, load,
):
    r = lax.axis_index("req")
    load_pool = pltpu.make_async_copy(cache, pool, load.at[0])
    load_pool.start()
    count = proj.shape[0]
    heads = QUERY_PER_KEY
    most_long = far_scores.shape[0]
    find_long(lengths, count, most_long, rank, at_long)
    pages = table.shape[0]
    channels = pool.shape[2]
    score_scale = 1.0 / math.sqrt(HEAD_SIZE)
    base = r * pool.shape[0]

    value = proj[...]
    lanes = lax.broadcasted_iota(jnp.int32, value.shape, 1)
    width = value.shape[1]
    first = (lanes % HEAD_SIZE) < HEAD_SIZE // 2
    partner = jnp.where(
        first,
        pltpu.roll(value, width - HEAD_SIZE // 2, axis=1),
        pltpu.roll(value, HEAD_SIZE // 2, axis=1),
    )
    repeat = width // cosines.shape[1]
    turned = value * jnp.concatenate([cosines[...]] * repeat, axis=1) + partner * jnp.concatenate(
        [sines[...]] * repeat, axis=1
    )
    key_at = heads * HEAD_SIZE
    rounded = jnp.where(lanes < key_at + HEAD_SIZE, turned, value).astype(BF).astype(F32)
    new_key = rounded[:, key_at : key_at + HEAD_SIZE]
    new_value = rounded[:, key_at + HEAD_SIZE :]
    queries[...] = jnp.zeros_like(queries)
    for h in range(heads):
        head = rounded[:, h * HEAD_SIZE : (h + 1) * HEAD_SIZE]
        queries[:, h, 0:HEAD_SIZE] = head
        own = jnp.sum(head * new_key, axis=1, keepdims=True) * score_scale
        owns[:, h, :] = jnp.broadcast_to(own, (count, channels))
    load_pool.wait()

    def entries(i, start, stop):
        return jnp.concatenate(
            [pool[jnp.clip(table[p, i] - base, 0, pool.shape[0] - 1)] for p in range(start, stop)], axis=0
        )

    def masked(raw, i, start):
        positions = lax.broadcasted_iota(jnp.int32, raw.shape, 1) + start
        return jnp.where(positions < lengths[i], raw * score_scale, LOWEST)

    at_once = 8 if count % 8 == 0 else 1

    def score(g, carry):
        for u in range(at_once):
            i = g * at_once + u
            scores[i] = masked(dot_nt(queries[i].astype(BF), entries(i, 0, SHORT_PAGES)), i, 0)
        return carry

    lax.fori_loop(0, count // at_once, score, 0)

    far_at_once = 4 if most_long % 4 == 0 else 1

    def far_score(g, carry):
        for u in range(far_at_once):
            j = g * far_at_once + u
            i = at_long[j]
            far_scores[j] = masked(dot_nt(queries[i].astype(BF), entries(i, SHORT_PAGES, pages)), i, SHORT_MAX)
        return carry

    lax.fori_loop(0, most_long // far_at_once, far_score, 0)

    def weigh(held, tops, bottoms):
        raw = held[...]
        top = jnp.max(raw, axis=2, keepdims=True)
        weight = jnp.exp(raw - top)
        held[...] = weight
        tops[...] = jnp.broadcast_to(top, tops.shape)
        bottoms[...] = jnp.broadcast_to(jnp.sum(weight, axis=2, keepdims=True), bottoms.shape)

    weigh(scores, tops, bottoms)
    weigh(far_scores, far_top, far_bottom)

    def mix(g, carry):
        for u in range(at_once):
            i = g * at_once + u
            mixed[i] = dot(scores[i].astype(BF), entries(i, 0, SHORT_PAGES))
        return carry

    lax.fori_loop(0, count // at_once, mix, 0)

    def far_mix(g, carry):
        for u in range(far_at_once):
            j = g * far_at_once + u
            far_mixed[j] = dot(far_scores[j].astype(BF), entries(at_long[j], SHORT_PAGES, pages))
        return carry

    lax.fori_loop(0, most_long // far_at_once, far_mix, 0)

    sink_rows = lax.broadcasted_iota(jnp.int32, (heads, channels), 0)
    sink = jnp.zeros((heads, channels), F32)
    for h in range(heads):
        sink = jnp.where(sink_rows == h, sinks[h], sink)

    def join(g, carry):
        for u in range(at_once):
            i = g * at_once + u
            k = rank[i]
            is_long = jnp.full((heads, channels), lengths[i], jnp.int32) > SHORT_MAX
            far = jnp.where(is_long, far_top[k], LOWEST)
            own = owns[i]
            near = tops[i]
            top = jnp.maximum(jnp.maximum(near, far), jnp.maximum(own, sink))
            near_scale = jnp.exp(near - top)
            far_scale = jnp.exp(far - top)
            own_weight = jnp.exp(own - top)
            bottom = bottoms[i] * near_scale + own_weight + jnp.exp(sink - top)
            bottom = bottom + jnp.where(is_long, far_bottom[k] * far_scale, 0.0)
            both = mixed[i] * near_scale + jnp.where(is_long, far_mixed[k] * far_scale, 0.0)
            mixed[i] = both / bottom
            owns[i] = own_weight / bottom
        return carry

    lax.fori_loop(0, count // at_once, join, 0)
    for h in range(heads):
        head = mixed[:, h, HEAD_SIZE:] + owns[:, h, 0:1] * new_value
        out[:, h * HEAD_SIZE : (h + 1) * HEAD_SIZE] = head.astype(BF)


def attend(lengths, table, proj, cosines, sines, sinks, cache):
    tokens = proj.shape[0]
    channels = cache.shape[2]
    pages = table.shape[0]
    most_long = tokens // 4
    vmem = pl.BlockSpec(memory_space=pltpu.VMEM)
    smem = pl.BlockSpec(memory_space=pltpu.SMEM)
    per_head = pltpu.VMEM((tokens, QUERY_PER_KEY, channels), F32)
    per_long = pltpu.VMEM((most_long, QUERY_PER_KEY, channels), F32)
    return pl.pallas_call(
        attend_kernel,
        name="attend",
        out_shape=jax.ShapeDtypeStruct((tokens, QUERY_PER_KEY * HEAD_SIZE), BF),
        in_specs=[smem, smem, vmem, vmem, vmem, smem, pl.BlockSpec(memory_space=pl.ANY)],
        out_specs=vmem,
        scratch_shapes=[
            pltpu.VMEM(cache.shape, BF),
            pltpu.SMEM((tokens,), jnp.int32),
            pltpu.SMEM((most_long,), jnp.int32),
            pltpu.VMEM((tokens, QUERY_PER_KEY, SHORT_PAGES * PAGE_POSITIONS), F32),
            pltpu.VMEM((most_long, QUERY_PER_KEY, (pages - SHORT_PAGES) * PAGE_POSITIONS), F32),
            *[per_head] * 5,
            *[per_long] * 3,
            pltpu.SemaphoreType.DMA((1,)),
        ],
        compiler_params=pltpu.CompilerParams(vmem_limit_bytes=VMEM_LIMIT),
    )(lengths, table, proj, cosines, sines, sinks, cache)


def expert_kernel(
    att, wo_all, hidden, obias, egain, router, router_bias, routes_t, w1_hbm, b1, w2_hbm, rbias,
    out,
    w1, w2, heads, halves, summed, mine, outgoing, gathered, full, pre, near_out, near_in, far_out, far_in,
    kept, back_out, back_in, logits_out, logits_in, share_f32, gains,
    x_send, x_recv, s_send, s_recv, d_send, d_recv, ring_send, ring_recv, p_send, p_recv,
    n_send, n_recv, f_send, f_recv, b_send, b_recv, l_send, l_recv, local,
):
    r, m, x, z, y, c = place()
    tokens, width = hidden.shape
    count_req, count_mdl = NX * NZ, NY * NC
    share = width // count_mdl
    block = width // count_req
    padded = outgoing.shape[2]
    rows = count_req * SLOTS
    per_group = NZ * block // share

    load1 = pltpu.make_async_copy(w1_hbm, w1, local.at[0])
    load2 = pltpu.make_async_copy(w2_hbm, w2, local.at[1])
    load1.start()
    load2.start()

    barrier = pltpu.get_barrier_semaphore()

    def greet(to_r, to_m):
        pl.semaphore_signal(barrier, inc=1, device_id=device(to_r, to_m), device_id_type=MESH)

    def greet_req(step, carry):
        greet((r + step) % count_req, m)
        return carry

    lax.fori_loop(1, count_req, greet_req, 0)
    for step in range(1, count_mdl):
        greet(r, (m + step) % count_mdl)
    diagonal = x == y
    for step in range(NX):
        for j in range(per_group):
            not_me = jnp.logical_or(step > 0, per_group * x + j != m)

            @pl.when(not_me)
            def _():
                greet((x + step) % NX * NZ + z, per_group * x + j)

    for j in range(count_mdl):

        @pl.when(jnp.logical_not(jnp.logical_and(diagonal, m == j)))
        def _():
            greet(y * NZ + z, j)

    pl.semaphore_wait(
        barrier,
        (count_req - 1) + (count_mdl - 1) + NX * per_group + count_mdl - 2 * diagonal.astype(jnp.int32),
    )

    for step in range(1, NX):
        to = (x + step) % NX
        remote(att, heads.at[x], x_send.at[step], x_recv.at[step], to * NZ + z, m).start()
    heads[x] = att[...]

    obias_row, egain_row = obias[...][None, :], egain[...][None, :]
    for k in range(count_mdl):

        @pl.when(m == k)
        def _():
            at = slice(share * k, share * k + share)
            share_f32[...] = hidden[:, at].astype(F32) + obias_row[:, at]
            gains[0:1, :] = egain_row[:, at]
            gains[8 : 8 + count_req, :] = rbias[:, at]
            gains[8 + count_req : 8 + 2 * count_req, :] = router[:, at].astype(F32)

    names = lax.broadcasted_iota(jnp.int32, (count_req, tokens), 0)
    hot_t = jnp.zeros((count_req, tokens), F32)
    for k in range(routes_t.shape[0]):
        hot_t = hot_t + (routes_t[k : k + 1, :] == names).astype(F32)
    same = lax.broadcasted_iota(jnp.int32, (tokens, tokens), 0) == lax.broadcasted_iota(
        jnp.int32, (tokens, tokens), 1
    )
    hot = dot_nt(same.astype(BF), hot_t.astype(BF))
    before = lax.broadcasted_iota(jnp.int32, (tokens, tokens), 0) < lax.broadcasted_iota(
        jnp.int32, (tokens, tokens), 1
    )
    rank_t = dot(hot_t.astype(BF), before.astype(BF))
    after = lax.broadcasted_iota(jnp.int32, (tokens, tokens), 0) > lax.broadcasted_iota(
        jnp.int32, (tokens, tokens), 1
    )
    rank = dot(after.astype(BF), hot.astype(BF))
    spread = (
        lax.broadcasted_iota(jnp.int32, (rows, count_req), 0) // SLOTS
        == lax.broadcasted_iota(jnp.int32, (rows, count_req), 1)
    ).astype(BF)
    spread_t = (
        lax.broadcasted_iota(jnp.int32, (count_req, rows), 1) // SLOTS
        == lax.broadcasted_iota(jnp.int32, (count_req, rows), 0)
    ).astype(BF)
    slot = (lax.broadcasted_iota(jnp.int32, (rows, tokens), 0) % SLOTS).astype(F32)
    place_rows = jnp.where(
        jnp.logical_and(dot(spread, hot_t.astype(BF)) > 0.5, dot(spread, rank_t.astype(BF)) == slot), 1.0, 0.0
    ).astype(BF)
    slot_t = (lax.broadcasted_iota(jnp.int32, (tokens, rows), 1) % SLOTS).astype(F32)
    take_rows = jnp.where(
        jnp.logical_and(dot(hot.astype(BF), spread_t) > 0.5, dot(rank.astype(BF), spread_t) == slot_t), 1.0, 0.0
    )

    for step in range(1, NX):
        origin = (x + NX - step) % NX
        remote(heads.at[origin], heads.at[origin], x_send.at[step], x_recv.at[step], r, m).wait_recv()

    stacked = jnp.concatenate([heads[j] for j in range(NX)], axis=0)
    per_share = share // block
    for k in range(NZ):
        product = dot_nt(stacked, wo_all[k]).astype(BF)
        for j in range(NX):
            halves[k // per_share, j, :, block * (k % per_share) : block * (k % per_share) + block] = product[
                j * tokens : (j + 1) * tokens
            ]

    def sum_copy(step, j):
        to = (x + step) % NX
        i = step * per_group + j
        return remote(
            halves.at[j, to], summed.at[m], s_send.at[i], s_recv.at[m], to * NZ + z, per_group * x + j
        )

    for step in range(NX):
        for j in range(per_group):

            @pl.when(jnp.logical_or(step > 0, per_group * x + j != m))
            def _():
                sum_copy(step, j).start()

    @pl.when(diagonal)
    def _():
        summed[m] = halves[m % per_group, x]

    residual = share_f32[...]
    for j in range(count_mdl):

        @pl.when(jnp.logical_not(jnp.logical_and(diagonal, m == j)))
        def _():
            remote(summed.at[j], summed.at[j], s_send.at[0], s_recv.at[j], r, m).wait_recv()

    total = summed[0].astype(F32)
    for j in range(1, count_mdl):
        total = total + summed[j].astype(F32)
    residual = (residual + total).astype(BF).astype(F32)
    share_f32[...] = residual
    squares = jnp.sum(residual * residual, axis=1, keepdims=True)
    scaled = (residual * gains[0:1, :]).astype(BF)
    mine[...] = jnp.zeros_like(mine)
    mine[:, 0:share] = scaled
    for k, piece in enumerate(split3(squares)):
        mine[:, share + k : share + k + 1] = piece

    outgoing[...] = dot(place_rows, mine[...]).astype(BF).reshape(outgoing.shape)

    def send_row(step, carry):
        to = (r + step) % count_req
        remote(outgoing.at[to], gathered.at[m, r], d_send.at[step], d_recv.at[r], to, m).start()
        return carry

    lax.fori_loop(1, count_req, send_row, 0)
    gathered[m, r] = outgoing[r]

    routing = gains[8 + count_req : 8 + 2 * count_req, :].astype(BF)
    logits_out[...] = jnp.zeros_like(logits_out)
    logits_out[:, 0:count_req] = dot_nt(scaled, routing)
    logits_out[:, count_req : count_req + 1] = squares
    for step in range(1, count_mdl):
        to = (m + step) % count_mdl
        remote(logits_out, logits_in.at[m], l_send.at[step], l_recv.at[step], r, to).start()
    logits_in[m] = logits_out[...]

    part_rows = count_req // 2

    def part_ref(origin, part):
        return gathered.at[origin * NC + c, pl.ds(part * part_rows, part_rows)]

    def at_y(to):
        return device(r, to * NC + c)

    ring = Ring(NY, y, part_ref, ring_send, ring_recv, at_y)

    def pair_index(way, dist):
        return way * ring.half + dist

    def pair_copy(way, dist, part):
        origin = ring.origin(way, dist)
        ref = part_ref(origin, part)
        i = pair_index(way, dist) * 2 + part
        return remote(ref, ref, p_send.at[i], p_recv.at[i], r, y * NC + 1 - c)

    def pair_arrive(way, dist, part):
        ref = gathered.at[ring.origin(way, dist) * NC + 1 - c, pl.ds(part * part_rows, part_rows)]
        i = pair_index(way, dist) * 2 + part
        remote(ref, ref, p_send.at[i], p_recv.at[i], r, m).wait_recv()

    for part in range(2):

        def take(origin, carry):
            @pl.when(origin != r)
            def _():
                remote(gathered.at[m, origin], gathered.at[m, origin], d_send.at[0], d_recv.at[origin], r, m).wait_recv()

            return carry

        lax.fori_loop(part * part_rows, (part + 1) * part_rows, take, 0)
        ring.begin(part)
        pair_copy(0, 0, part).start()

    for way, dist, part in ring.plan:
        ring.step(way, dist, part)
        pair_copy(way, dist, part).start()
    pair_plan = [(0, 0, 0), (0, 0, 1)] + ring.plan
    for way, dist, part in pair_plan:
        pair_arrive(way, dist, part)

    load1.wait()
    load2.wait()
    square_sum = jnp.zeros((rows, 1), F32)
    for k in range(count_mdl):
        piece = gathered[k].reshape(rows, padded)
        full[:, share * k : share * k + share] = piece[:, 0:share]
        for j in range(3):
            square_sum = square_sum + piece[:, share + j : share + j + 1].astype(F32)
    root = lax.rsqrt(square_sum * (1.0 / width) + norm_epsilon)
    columns = w1.shape[0]
    pre[...] = jnp.zeros_like(pre)
    pre[:, 0:columns] = dot_nt(full[...], w1[...]) * root + b1[...]
    raw = pre[...]
    up = jnp.clip(pltpu.roll(raw, raw.shape[1] - 1, axis=1), -swiglu_limit, swiglu_limit)
    gate = jnp.minimum(raw, swiglu_limit)
    act = (gate * jax.nn.sigmoid(swiglu_alpha * gate) * (up + 1.0)).astype(BF)
    hidden_units = columns // 2
    pick = (
        lax.broadcasted_iota(jnp.int32, (raw.shape[1], hidden_units), 0)
        == 2 * lax.broadcasted_iota(jnp.int32, (raw.shape[1], hidden_units), 1)
    ).astype(BF)
    act = dot(act, pick).astype(BF)

    def produce(k):
        return dot(act, w2[:, share * k : share * k + share])

    def near_copy(k):
        return remote(near_out.at[k], near_in.at[k], n_send.at[k], n_recv.at[k], r, y * NC + 1 - c)

    for core in range(NC):

        @pl.when(c == core)
        def _():
            for k in range(NY):
                near_out[k] = produce(k * NC + 1 - core).astype(BF)
                near_copy(k).start()
            for k in range(NY):
                kept[k] = produce(k * NC + core)

    def far_copy(step):
        to = (y + step) % NY
        return remote(far_out.at[to], far_in.at[y], f_send.at[step], f_recv.at[step], r, to * NC + c)

    for step in range(1, NY):
        to = (y + step) % NY
        remote(near_in.at[to], near_in.at[to], n_send.at[to], n_recv.at[to], r, m).wait_recv()
        far_out[to] = (kept[to] + near_in[to].astype(F32)).astype(BF)
        far_copy(step).start()
    remote(near_in.at[y], near_in.at[y], n_send.at[y], n_recv.at[y], r, m).wait_recv()
    answer = kept[y] + near_in[y].astype(F32)
    for step in range(1, NY):
        origin = (y + NY - step) % NY
        remote(far_in.at[origin], far_in.at[origin], f_send.at[step], f_recv.at[step], r, m).wait_recv()
        answer = answer + far_in[origin].astype(F32)
    back_out[...] = answer.astype(BF).reshape(back_out.shape)

    def send_back(step, carry):
        to = (r + step) % count_req
        remote(back_out.at[to], back_in.at[r], b_send.at[step], b_recv.at[step], to, m).start()
        return carry

    lax.fori_loop(1, count_req, send_back, 0)
    back_in[r] = back_out[r]

    for step in range(1, count_mdl):
        origin = (m + count_mdl - step) % count_mdl
        remote(logits_in.at[origin], logits_in.at[origin], l_send.at[step], l_recv.at[step], r, m).wait_recv()
    both = logits_in[0]
    for k in range(1, count_mdl):
        both = both + logits_in[k]
    row_root = lax.rsqrt(both[:, count_req : count_req + 1] * (1.0 / width) + norm_epsilon)
    logits = both[:, 0:count_req] * row_root + router_bias[...]
    logits = jnp.where(hot > 0.5, logits, -jnp.inf)
    weight = jnp.exp(logits - jnp.max(logits, axis=1, keepdims=True))
    gates = weight / jnp.sum(weight, axis=1, keepdims=True)
    result = share_f32[...]
    biases = split3(gains[8 : 8 + count_req, :])
    gate_parts = split3(gates)
    for i in range(3):
        for j in range(3 - i):
            result = result + dot(gate_parts[i], biases[j])
    takers = [(take_rows * dot(piece, spread_t)).astype(BF) for piece in gate_parts]

    def take_back(step, carry):
        origin = (r + count_req - step) % count_req
        remote(back_in.at[origin], back_in.at[origin], b_send.at[step], b_recv.at[step], r, m).wait_recv()
        return carry

    lax.fori_loop(1, count_req, take_back, 0)
    returned = back_in[...].reshape(rows, share)
    for taker in takers:
        result = result + dot(taker, returned)
    out[...] = result.astype(BF)

    for step in range(1, NX):
        to = (x + step) % NX
        remote(att, heads.at[x], x_send.at[step], x_recv.at[step], to * NZ + z, m).wait_send()
    for step in range(NX):
        for j in range(per_group):

            @pl.when(jnp.logical_or(step > 0, per_group * x + j != m))
            def _():
                sum_copy(step, j).wait_send()

    def sent(step, carry):
        to = (r + step) % count_req
        remote(outgoing.at[to], gathered.at[m, r], d_send.at[step], d_recv.at[r], to, m).wait_send()
        remote(back_out.at[to], back_in.at[r], b_send.at[step], b_recv.at[step], to, m).wait_send()
        return carry

    lax.fori_loop(1, count_req, sent, 0)
    ring.finish()
    for way, dist, part in pair_plan:
        pair_copy(way, dist, part).wait_send()
    for k in range(NY):
        near_copy(k).wait_send()
    for step in range(1, NY):
        far_copy(step).wait_send()
    for step in range(1, count_mdl):
        to = (m + step) % count_mdl
        remote(logits_out, logits_in.at[m], l_send.at[step], l_recv.at[step], r, to).wait_send()


def experts(att, wo_all, hidden, obias, egain, router, router_bias, routes_t, w1, b1, w2, rbias):
    tokens, width = hidden.shape
    count_req, count_mdl = NX * NZ, NY * NC
    share = width // count_mdl
    padded = -(-(share + 3) // 128) * 128
    rows = count_req * SLOTS
    columns = w1.shape[0]
    wide = -(-(columns + 1) // 128) * 128
    per_group = count_mdl // NX
    vmem = pl.BlockSpec(memory_space=pltpu.VMEM)
    hbm = pl.BlockSpec(memory_space=pl.ANY)
    dma = pltpu.SemaphoreType.DMA
    return pl.pallas_call(
        expert_kernel,
        name="experts",
        out_shape=jax.ShapeDtypeStruct((tokens, share), BF),
        in_specs=[vmem] * 8 + [hbm, vmem, hbm, vmem],
        out_specs=vmem,
        scratch_shapes=[
            pltpu.VMEM(w1.shape, BF),
            pltpu.VMEM(w2.shape, BF),
            pltpu.VMEM((NX,) + att.shape, BF),
            pltpu.VMEM((per_group, NX, tokens, share), BF),
            pltpu.VMEM((count_mdl, tokens, share), BF),
            pltpu.VMEM((tokens, padded), BF),
            pltpu.VMEM((count_req, SLOTS, padded), BF),
            pltpu.VMEM((count_mdl, count_req, SLOTS, padded), BF),
            pltpu.VMEM((rows, width), BF),
            pltpu.VMEM((rows, wide), F32),
            pltpu.VMEM((NY, rows, share), BF),
            pltpu.VMEM((NY, rows, share), BF),
            pltpu.VMEM((NY, rows, share), BF),
            pltpu.VMEM((NY, rows, share), BF),
            pltpu.VMEM((NY, rows, share), F32),
            pltpu.VMEM((count_req, SLOTS, share), BF),
            pltpu.VMEM((count_req, SLOTS, share), BF),
            pltpu.VMEM((tokens, 128), F32),
            pltpu.VMEM((count_mdl, tokens, 128), F32),
            pltpu.VMEM((tokens, share), F32),
            pltpu.VMEM((8 + 2 * count_req, share), F32),
            dma((NX,)), dma((NX,)),
            dma((NX * per_group,)), dma((count_mdl,)),
            dma((count_req,)), dma((count_req,)),
            *ring_sems(NY),
            dma((2 * (NY + 2),)), dma((2 * (NY + 2),)),
            dma((NY,)), dma((NY,)),
            dma((NY,)), dma((NY,)),
            dma((count_req,)), dma((count_req,)),
            dma((count_mdl,)), dma((count_mdl,)),
            dma((2,)),
        ],
        compiler_params=pltpu.CompilerParams(
            collective_id=2, has_side_effects=True, vmem_limit_bytes=VMEM_LIMIT
        ),
    )(att, wo_all, hidden, obias, egain, router, router_bias, routes_t, w1, b1, w2, rbias)


def rotation_tables(lengths, repeat):
    half = HEAD_SIZE // 2
    frequency = np.power(rope_theta, -np.arange(half) * (2.0 / HEAD_SIZE))
    frequency = np.tile(frequency, 2 * repeat).astype(np.float32)
    sign = np.tile(np.repeat(np.float32([-1.0, 1.0]), half), repeat)
    angles = lengths.astype(F32)[:, None] * frequency[None, :]
    return jnp.cos(angles), jnp.sin(angles) * sign[None, :]


def shards(
    hidden_state,
    cached_length_list,
    page_table,
    paged_cache_store,
    attention_gain,
    qkv_weight,
    qkv_bias,
    sink_logit_values,
    output_weight,
    output_bias,
    expert_gain,
    router_weight,
    router_bias,
    expert_routes,
    expand_weight,
    expand_bias,
    reduce_weight,
    reduce_bias,
):
    projected, wo_all = project(
        hidden_state, attention_gain, qkv_weight, output_weight.T, qkv_bias
    )
    cosines, sines = rotation_tables(cached_length_list, 2)
    attended = attend(
        cached_length_list, page_table.T, projected, cosines, sines, sink_logit_values, paged_cache_store
    )
    return experts(
        attended,
        wo_all,
        hidden_state,
        output_bias,
        expert_gain,
        router_weight.T,
        router_bias[None],
        expert_routes.T,
        expand_weight[0].T,
        expand_bias,
        reduce_weight[0],
        reduce_bias,
    )


def solution(mesh):
    in_specs = (
        P("req", None),
        P("req"),
        P("req", None),
        P("req", None, "mdl"),
        P(),
        P("req", "mdl"),
        P("mdl"),
        P("mdl"),
        P("mdl", "req"),
        P(),
        P(),
        P(),
        P(),
        P("req", None),
        P("req", None, "mdl"),
        P("req", "mdl"),
        P("req", "mdl", None),
        P(),
    )
    out_specs = P("req", "mdl")
    return jax.shard_map(shards, mesh=mesh, in_specs=in_specs, out_specs=out_specs, check_vma=False)
```
